32 devices in a mesh: tm: 2 (over x), lat: 4 (over y, core), lon: 4 (over z).
Axes of the slice: x: 2, y: 2, z: 4, core: 2. Of those that a mesh axis runs over, the one named last changes fastest.
Arguments:
- forcing: float32 [8, 512, 2048], P('tm', 'lat', 'lon'), may hold values from -17 to 17
- depth: float32 [512, 2048], P('lat', 'lon'), may hold values from 0.2 to 2
- mask: int32 [512, 2048], P('lat', 'lon'), may hold values 0 or 1
- guess: float32 [2, 512, 2048], P('tm', 'lat', 'lon'), may hold values from -6 to 6
Outputs:
- adjoint: float32 [8, 512, 2048], P('tm', 'lat', 'lon')
The draws below stay inside these ranges and needn't reach their ends.
All inputs are finite; a program needn't handle non-finite values. No bound on the sum of `mask` on one device may be relied on, other than what follows from the above.
Results may differ from the reference program's by a relative error of at most 0.0001.
Values sent between devices are 32-bit elements; how exact they have to be, the bound alone decides.
No kernel may reach another device: no remote copies, remote signals or barrier semaphores. Data moves between devices by JAX's collectives and lax.ppermute only.
A program may use at most 64 MiB of HBM per device.

```python
import math
import jax
import jax.numpy as jnp
from jax import lax

FS = 4
FINE_ITERS = 2
NLAT = 512
NLON = 2048
NSTEPS = 8
N_TM = 2


def draw_forcing(key, part):
    lat_pos = jnp.arange(NLAT, dtype=jnp.float32) / (NLAT - 1)
    lon_pos = jnp.arange(NLON, dtype=jnp.float32) / (NLON - 1)
    scale = (0.5 * 3.0 ** lat_pos)[:, None] * (1.0 + 2.0 * lon_pos)[None, :]
    noise = jax.random.truncated_normal(key, -3.0, 3.0, (NSTEPS, NLAT, NLON), jnp.float32)
    return noise * scale[None]


def with_ends(values, stream_key, least, high):
    place = [jax.random.randint(jax.random.fold_in(stream_key, axis), (), 0, length) for axis, length in enumerate(values.shape)]
    main_axis = values.shape.index(max(values.shape))
    beside = place[:main_axis] + [(place[main_axis] + 1) % values.shape[main_axis]] + place[main_axis + 1:]
    return values.at[tuple(place)].set(least).at[tuple(beside)].set(high)


def shard_levels(key, shape, shards, least, largest):
    def one(dim, shards_of):
        draws = jax.random.uniform(jax.random.fold_in(jax.random.fold_in(key, 6), dim), (shards_of,), jnp.float32, least / len(shards), largest / len(shards))
        return jnp.repeat(jnp.exp(draws), shape[dim] // shards_of).reshape((-1,) + (1,) * (len(shape) - dim - 1))

    factor_of = one(*shards[0])
    for cut in shards[1:]:
        factor_of = factor_of * one(*cut)
    return factor_of


def normal_values(own_key, extent, deviation, most, shards=(), kind=jnp.bfloat16):
    loudness = shard_levels(own_key, extent, shards, -0.22, 0.18) if shards else 1.0
    drawn = jax.random.normal(own_key, extent, jnp.float32) * deviation * loudness
    return jnp.minimum(jnp.maximum(drawn, -most), most).astype(kind)


def setup_inputs(seed: int = 0) -> dict:
    streams_of = jax.random.split(jax.random.key(seed), 5)
    return {
        "forcing": draw_forcing(jax.random.fold_in(streams_of[4], 71), 0),
        "depth": jnp.clip(jnp.exp(math.log(2.0) - 2.3025851 * jax.random.uniform(streams_of[1], (NLAT, NLON), jnp.float32) ** shard_levels(streams_of[1], (NLAT, NLON), ((0, 4), (1, 4)), -0.2, 0.2)), 0.2, 2.0),
        "mask": with_ends((jax.random.randint(streams_of[2], (NLAT, NLON), 0, 10) < 7).astype(jnp.int32), jax.random.fold_in(streams_of[2], 1), 0, 1),
        "guess": normal_values(streams_of[3], (N_TM, NLAT, NLON), 1.0, 6.0, ((0, 2), (1, 4), (2, 4)), jnp.float32),
    }


COUPLING = 3.0
EPSILON = 1e-6


def face_terms(depth, mask):
    wet = mask.astype(jnp.float32)
    east = COUPLING * wet * jnp.roll(wet, -1, 1) * 0.5 * (depth + jnp.roll(depth, -1, 1))
    north = COUPLING * wet[:-1] * wet[1:] * 0.5 * (depth[:-1] + depth[1:])
    return east, north


def apply_op(field, east, north, factor):
    flux_east = east * (field - jnp.roll(field, -1, 1))
    spread = flux_east - jnp.roll(flux_east, 1, 1)
    flux_north = north * (field[:-1] - field[1:])
    zero_row = jnp.zeros((1, field.shape[1]), jnp.float32)
    spread = spread + jnp.concatenate([flux_north, zero_row], 0) - jnp.concatenate([zero_row, flux_north], 0)
    return field + factor * spread


def solve(source, east, north, factor, count):
    solution = jnp.zeros_like(source)
    residual = source
    direction = source
    norm_now = jnp.sum(residual * residual)
    for level in range(count):
        image = apply_op(direction, east, north, factor)
        alpha = norm_now / (jnp.sum(direction * image) + EPSILON)
        solution = solution + alpha * direction
        residual = residual - alpha * image
        if level + 1 < count:
            norm_next = jnp.sum(residual * residual)
            direction = residual + (norm_next / (norm_now + EPSILON)) * direction
            norm_now = norm_next
    return solution


def reference(forcing, depth, mask, guess):
    east, north = face_terms(depth, mask)

    def fine(value):
        return solve(value, east, north, 1.0, FINE_ITERS)

    def coarse(value):
        return solve(value, east, north, float(FS), 1)

    slabs = forcing.reshape(N_TM, FS, NLAT, NLON)
    empty = jnp.zeros((), jnp.float32)

    def relax(carry, inputs):
        start, terms = inputs
        value = start
        for level in range(FS - 1, 0, -1):
            value = fine(value) + terms[level]
        finished = fine(value) + terms[0]
        return carry, finished - coarse(start)

    _, offsets = lax.scan(relax, empty, (guess, slabs))

    def chain(upper, offset):
        here = coarse(upper) + offset
        return here, (upper, here)

    _, (uppers, heres) = lax.scan(chain, guess[N_TM - 1], offsets, reverse=True)

    def correct(carry, inputs):
        upper, here, terms = inputs
        value = upper
        later = []
        for level in range(FS - 1, 0, -1):
            value = fine(value) + terms[level]
            later.append(value)
        return carry, jnp.stack([here] + later[::-1])

    _, result = lax.scan(correct, empty, (uppers, heres, slabs))
    return result.reshape(NSTEPS, NLAT, NLON)
```

```python
import functools
import jax
import jax.numpy as jnp
from jax import lax
from jax.experimental import pallas as pl
from jax.experimental.pallas import tpu as pltpu
from jax.sharding import PartitionSpec as P

FS = 4
COUPLING = 3.0
EPSILON = 1e-06
HALO = 8
TOP = 2 * HALO

LENGTHS_RELAX = {
    (i, j): (2 * (FS + 1) - i - j if i or j else 2 * FS + 2) for i in range(FS + 1) for j in range(i, FS + 1)
}
LENGTHS_CORRECT = {(0, j): 2 * FS - j for j in range(FS - 1)}
SPARE = 64


def offsets_of(lengths):
    places, at = {}, 0
    for pair, length in lengths.items():
        places[pair] = at
        at += length
    return places


PLACES_RELAX = offsets_of(LENGTHS_RELAX)
PLACES_CORRECT = offsets_of(LENGTHS_CORRECT)


def two_sum(a, b):
    s = a + b
    t = s - a
    return s, (a - (s - t)) + (b - t)


def quick_sum(a, b):
    s = a + b
    return s, b - (s - a)


def pair_add(x, y):
    s, e = two_sum(x[0], y[0])
    return quick_sum(s, e + (x[1] + y[1]))


def split(a):
    t = 4097.0 * a
    hi = t - (t - a)
    return hi, a - hi


def pair_scale(x, d):
    p = x[0] * d
    ah, al = split(x[0])
    bh, bl = split(d)
    e = ((ah * bh - p) + ah * bl + al * bh) + al * bl
    return quick_sum(p, e + x[1] * d)


def tree(items):
    while len(items) > 1:
        items = [pair_add(items[i], items[i + 1]) if i + 1 < len(items) else items[i] for i in range(0, len(items), 2)]
    return items[0]


def roll_pair(x, shift, axis):
    return tuple(pltpu.roll(part, shift, axis) for part in x)


def spread_first(x):
    return jnp.broadcast_to(x[0:1, 0:1], (8, 128))


def lap_rows(src, east, north, row):
    count = east.shape[0]
    lane = lax.broadcasted_iota(jnp.int32, (8, 128), 1)
    last, first = lane == 127, lane == 0
    v = [src[c, pl.ds(row, 8), :] for c in range(count)]
    turned = [pltpu.roll(x, 127, 1) for x in v]
    flux = [
        east[c, pl.ds(row, 8), :] * (v[c] - jnp.where(last, turned[(c + 1) % count], turned[c])) for c in range(count)
    ]
    back = [pltpu.roll(x, 1, 1) for x in flux]
    out = []
    for c in range(count):
        below = north[c, pl.ds(row, 8), :] * (v[c] - src[c, pl.ds(row + 1, 8), :])
        above = north[c, pl.ds(row - 1, 8), :] * (src[c, pl.ds(row - 1, 8), :] - v[c])
        out.append(flux[c] - jnp.where(first, back[(c - 1) % count], back[c]) + below - above)
    return out


def row_loop(start, stop, body):
    def turn(i, carry):
        body(pl.multiple_of(i * 8, 8))
        return carry

    lax.fori_loop(start // 8, stop // 8, turn, 0)


def zero_spare(ref, lead, rows):
    for k in range(lead):
        for c in range(ref.shape[1]):
            ref[k, c, pl.ds(0, 8), :] = jnp.zeros((8, 128), jnp.float32)
            ref[k, c, pl.ds(rows - 8, 8), :] = jnp.zeros((8, 128), jnp.float32)


def dot_groups(acc, groups, load, rows, tiles):
    for group in groups:
        keys = sorted({k for _, a, b in group for k in (a, b)})

        def body(i, carry):
            row = pl.multiple_of(i * 8, 8)
            for c in range(tiles):
                held = {k: load(k, c, row) for k in keys}
                carry = tuple(old + held[a] * held[b] for old, (_, a, b) in zip(carry, group))
            return carry

        sums = lax.fori_loop(
            0, rows // 8, body, tuple(jnp.zeros((8, 128), jnp.float32) for _ in group)
        )
        for total, (m, _, _) in zip(sums, group):
            acc[pl.ds(8 * m, 8), :] = total


def reduce_acc(acc, count, out_ref):
    zero = jnp.zeros((128, 128), jnp.float32)
    for m in range(count, 128):
        acc[pl.ds(8 * m, 8), :] = jnp.zeros((8, 128), jnp.float32)
    hi, lo = tree([(acc[pl.ds(s, 128, stride=8), :], zero) for s in range(8)])
    hi, lo = hi.T, lo.T
    both = tree([(hi[8 * k : 8 * k + 8], lo[8 * k : 8 * k + 8]) for k in range(16)])
    for shift in (4, 2, 1):
        both = pair_add(both, roll_pair(both, shift, 0))
    sub = lax.broadcasted_iota(jnp.int32, (8, 128), 0)
    block = jnp.where(sub == 0, both[0], jnp.where(sub == 1, both[1], 0.0))
    for k in range(out_ref.shape[0]):
        out_ref[k] = block


def gather_sum(ref):
    rows = [(ref[k, 0:1, :], ref[k, 1:2, :]) for k in range(ref.shape[0])]
    hi, lo = tree(rows)
    return jnp.broadcast_to(hi, (8, 128)), jnp.broadcast_to(lo, (8, 128))


def rows_of(moments, places):
    sub = lax.broadcasted_iota(jnp.int32, (8, 128), 0)
    out = []
    for part in moments:
        built = jnp.zeros((8, 128), jnp.float32)
        for row, at in places.items():
            moved = pltpu.roll(part, (128 - at) % 128, 1) if at else part
            built = jnp.where(sub == row, moved, built)
        out.append(built)
    return tuple(out)


def fine_factors(n0, n1, n2, n3):
    den = n0 + n1 + EPSILON
    a0 = n0 / den
    left = (n1 + EPSILON) / den
    s1 = jnp.maximum(left * left * n0 - 2.0 * left * a0 * n1 + a0 * a0 * n2, 0.0)
    big = left + s1 / (n0 + EPSILON)
    small = -a0
    curve = big * big * (n0 + n1) + 2.0 * big * small * (n1 + n2) + small * small * (n2 + n3)
    a1 = jnp.clip(s1 / (curve + EPSILON), 0.0, 1.0)
    return a0 + a1 * big, a1 * small


def coarse_factor(state):
    n0 = state[0]
    n1 = pltpu.roll(n0, 127, 1)
    return spread_first(n0 / (n0 + FS * n1 + EPSILON))


def factors_of(state):
    n0 = state[0]
    d0, d1 = fine_factors(n0, pltpu.roll(n0, 127, 1), pltpu.roll(n0, 126, 1), pltpu.roll(n0, 125, 1))
    return spread_first(d0), spread_first(d1)


def advance(state, gram, step, factors):
    d0, d1 = factors
    sub = lax.broadcasted_iota(jnp.int32, (8, 128), 0)

    def mixed(x, plus):
        moved = pair_add(pair_scale(x, d0), pair_scale(roll_pair(x, 127, 1), d1))
        return pair_add(moved, plus)

    def row(x, r):
        return tuple(jnp.broadcast_to(part[r : r + 1, :], (8, 128)) for part in x)

    cross = row(state, step)
    plus = tuple(jnp.where(sub == 0, a, b) for a, b in zip(cross, gram))
    half = mixed(state, plus)
    full = mixed(half, row(half, step))
    return tuple(jnp.where(sub == 0, a, b) for a, b in zip(full, half))


def gram_rows(moments, step, last):
    return rows_of(moments, {h: PLACES_RELAX[step, h] for h in range(step, last + 1)})


def pack_kernel(fields, depth, mask, forcing, guess, low_in, high_in, low_out, high_out):
    lat_odd = lax.rem(lax.axis_index("lat"), 2) == 1
    lon_odd = lax.rem(lax.axis_index("lon"), 2) == 1
    rows, cols = depth.shape
    tiles = rows // 8 + 2
    lane = lax.broadcasted_iota(jnp.int32, (8, 128), 1) // 8
    edges = []
    for start in (cols - 128, 0):
        window = pl.ds(start, 128)

        def tile(f, t):
            if t in (0, tiles - 1):
                a, b = low_in[pl.ds(8 * f, 8), window], high_in[pl.ds(8 * f, 8), window]
                return jnp.where(lat_odd, a, b) if t == 0 else jnp.where(lat_odd, b, a)
            own = pl.ds(8 * (t - 1), 8)
            if f == 0:
                return jnp.where(mask[own, window] > 0, depth[own, window], 0.0)
            if f == 1:
                return guess[0, own, window]
            return forcing[FS + 1 - f, own, window]

        packed = [jnp.zeros((8, 128), jnp.float32) for _ in range(-(-fields * tiles // 16))]
        for f in range(fields):
            for t in range(tiles):
                at, slot = divmod(f * tiles + t, 16)
                shift = (8 * slot + (8 if start else 0)) % 128
                value = tile(f, t)
                value = pltpu.roll(value, shift, 1) if shift else value
                packed[at] = jnp.where(lane == slot, value, packed[at])
        edges.append(packed)
    for k, (e, w) in enumerate(zip(*edges)):
        low_out[pl.ds(8 * k, 8), :] = jnp.where(lon_odd, w, e)
        high_out[pl.ds(8 * k, 8), :] = jnp.where(lon_odd, e, w)


def relax_kernel(depth, mask, forcing, guess, low_in, high_in, low_col, high_col, held, extra, sums, kry, wet, acc):
    lat_odd = lax.rem(lax.axis_index("lat"), 2) == 1
    lon_odd = lax.rem(lax.axis_index("lon"), 2) == 1
    rows, cols = depth.shape
    own = cols // 128
    count = own + 1
    tiles = rows // 8 + 2
    total = rows + 4 * HALO
    lane = lax.broadcasted_iota(jnp.int32, (8, 128), 1)
    fields = FS + 2
    zero = jnp.zeros((8, 128), jnp.float32)

    def put(f, c, row, value):
        if f == 0:
            wet[c, pl.ds(row, 8), :] = value
        else:
            kry[start_of[f - 1], c, pl.ds(row, 8), :] = value
            held[1 + f, c, pl.ds(row, 8), :] = value

    start_of, at = {}, 0
    for s in range(FS + 1):
        start_of[s] = at
        at += FS + 2 - s
    zero_spare(kry, at, total)
    for c in range(count):
        for row in (0, total - 8):
            wet[c, pl.ds(row, 8), :] = zero
            for k in range(fields + 1):
                held[k, c, pl.ds(row, 8), :] = zero
    for f in range(fields):
        for c in range(own):
            window = pl.ds(128 * c, 128)
            a, b = low_in[pl.ds(8 * f, 8), window], high_in[pl.ds(8 * f, 8), window]
            put(f, c, TOP - 8, jnp.where(lat_odd, a, b))
            put(f, c, TOP + rows, jnp.where(lat_odd, b, a))
        for t in range(tiles):
            k, slot = divmod(f * tiles + t, 16)
            a, b = low_col[pl.ds(8 * k, 8), :], high_col[pl.ds(8 * k, 8), :]
            e, w = jnp.where(lon_odd, b, a), jnp.where(lon_odd, a, b)
            e = pltpu.roll(e, 128 - 8 * slot, 1) if slot else e
            w = pltpu.roll(w, (120 - 8 * slot) % 128, 1) if slot < 15 else w
            put(f, own, TOP - 8 + 8 * t, jnp.where(lane < 8, e, jnp.where(lane >= 120, w, 0.0)))

    def fill(row):
        from_row = pl.ds(pl.multiple_of(row - TOP, 8), 8)
        for c in range(own):
            window = pl.ds(128 * c, 128)
            put(0, c, row, jnp.where(mask[from_row, window] > 0, depth[from_row, window], 0.0))
            put(1, c, row, guess[0, from_row, window])
            for f in range(2, fields):
                put(f, c, row, forcing[FS + 1 - f, from_row, window])

    row_loop(TOP, TOP + rows, fill)

    def faces(row):
        d = [wet[c, pl.ds(row, 8), :] for c in range(count)]
        turned = [pltpu.roll(x, 127, 1) for x in d]
        for c in range(count):
            right = jnp.where(lane == 127, turned[(c + 1) % count], turned[c])
            under = wet[c, pl.ds(row + 1, 8), :]
            half = COUPLING * 0.5
            held[0, c, pl.ds(row, 8), :] = jnp.where((d[c] > 0) & (right > 0), half * (d[c] + right), 0.0)
            held[1, c, pl.ds(row, 8), :] = jnp.where((d[c] > 0) & (under > 0), half * (d[c] + under), 0.0)

    row_loop(8, total - 8, faces)
    east, north = held.at[0], held.at[1]

    for degree in range(FS + 1):
        def power(row, degree=degree):
            for s in range(FS + 1 - degree):
                at = start_of[s] + degree
                for c, value in enumerate(lap_rows(kry.at[at], east, north, row)):
                    kry[at + 1, c, pl.ds(row, 8), :] = value

        row_loop(8, total - 8, power)

    def copy(row):
        to_row = pl.ds(pl.multiple_of(row - TOP, 8), 8)
        for k, (s, degree) in enumerate(EXTRA):
            for c in range(own):
                extra[k, c, to_row, :] = kry[start_of[s] + degree, c, pl.ds(row, 8), :]

    row_loop(TOP, TOP + rows, copy)

    groups, group = [], []
    for (i, j), length in LENGTHS_RELAX.items():
        if len(group) + length > 26:
            groups.append(group)
            group = []
        for k in range(length):
            b = min(k // 2, FS + 1 - j)
            group.append((PLACES_RELAX[i, j] + k, start_of[i] + k - b, start_of[j] + b))
    groups.append(group)
    dot_groups(acc, groups, lambda k, c, row: kry[k, c, pl.ds(row + TOP, 8), :], rows, own)
    reduce_acc(acc, sum(LENGTHS_RELAX.values()), sums)


EXTRA = ((1, 1), (1, 2), (2, 1))


def slab_kernel(gathered, held, here, offset, kept, one, two):
    rows = held.shape[2]
    count = held.shape[1]
    lane = lax.broadcasted_iota(jnp.int32, (8, 128), 1)
    sub = lax.broadcasted_iota(jnp.int32, (8, 128), 0)
    moments = gather_sum(gathered)
    state = rows_of(moments, {j: PLACES_RELAX[0, j] for j in range(FS + 1)})
    down = coarse_factor(state)
    steps = []
    for step in range(1, FS + 1):
        factors = factors_of(state)
        steps.append(factors)
        state = advance(state, gram_rows(moments, step, FS), step, factors)
    sent = coarse_factor(state)
    kept[...] = jnp.where(sub == 0, moments[0], jnp.where(sub == 1, moments[1], jnp.where(sub == 2, down, 0.0)))
    east, north = held.at[0], held.at[1]
    for ref in (one, two):
        zero_spare(ref, 1, rows)
    zero = jnp.zeros((8, 128), jnp.float32)
    for c in range(count):
        for row in (0, rows - 8):
            here[c, pl.ds(row, 8), :] = zero
            offset[c, pl.ds(row, 8), :] = zero
    sources = [held.at[2], one.at[0], two.at[0], one.at[0]]
    targets = [one.at[0], two.at[0], one.at[0], None]
    for step, (d0, d1) in enumerate(steps):
        def move(row, step=step, d0=d0, d1=d1):
            for c, value in enumerate(lap_rows(sources[step], east, north, row)):
                window = pl.ds(row, 8)
                value = d0 * sources[step][c, window, :] + d1 * value + held[3 + step, c, window, :]
                if targets[step] is not None:
                    targets[step][c, window, :] = value
                else:
                    coarse = down * held[2, c, window, :]
                    rest = value - coarse
                    offset[c, window, :] = rest
                    value = coarse + rest
                    if c == count - 1:
                        value = jnp.where(lane == SPARE, sent, value)
                    here[c, window, :] = value

        row_loop(8, rows - 8, move)


def moment_kernel(moved, held, extra, upper, sums, kry, acc):
    is_final = lax.axis_index("tm") == lax.axis_size("tm") - 1
    rows, count = held.shape[2], held.shape[1]
    own_rows, own = extra.shape[2], extra.shape[1]
    zero_spare(kry, FS + 1, rows)
    zero = jnp.zeros((8, 128), jnp.float32)
    for c in range(count):
        for row in (0, rows - 8):
            upper[c, pl.ds(row, 8), :] = zero

    def choose(row):
        for c in range(count):
            window = pl.ds(row, 8)
            value = jnp.where(is_final, held[2, c, window, :], moved[c, window, :])
            upper[c, window, :] = value
            kry[0, c, window, :] = value

    row_loop(8, rows - 8, choose)
    for degree in range(FS):
        def power(row, degree=degree):
            for c, value in enumerate(lap_rows(kry.at[degree], held.at[0], held.at[1], row)):
                kry[degree + 1, c, pl.ds(row, 8), :] = value

        row_loop(8, rows - 8, power)

    def load(key, c, row):
        s, degree = key
        if s == 0:
            return kry[degree, c, pl.ds(row + TOP, 8), :]
        if degree == 0:
            return held[2 + s, c, pl.ds(row + TOP, 8), :]
        return extra[EXTRA.index(key), c, pl.ds(row, 8), :]

    group = []
    for (i, j), length in LENGTHS_CORRECT.items():
        for k in range(length):
            b = max(k - FS, 0) if j else k // 2
            group.append((PLACES_CORRECT[i, j] + k, (0, k - b), (j, b)))
    dot_groups(acc, [group], load, own_rows, own)
    reduce_acc(acc, sum(LENGTHS_CORRECT.values()), sums)


def correct_kernel(gathered, kept, upper, held, offset, out, one, two):
    is_final = lax.axis_index("tm") == lax.axis_size("tm") - 1
    rows, count = held.shape[2], held.shape[1]
    own_rows, own = out.shape[1], out.shape[2] // 128
    moments = gather_sum(gathered)
    before = tuple(jnp.broadcast_to(kept[k : k + 1, :], (8, 128)) for k in range(2))
    state = rows_of(moments, {j: PLACES_CORRECT[0, j] for j in range(FS - 1)})
    steps = []
    for step in range(1, FS):
        factors = factors_of(state)
        steps.append(factors)
        if step < FS - 1:
            state = advance(state, gram_rows(before, step, FS - 2), step, factors)
    down = jnp.broadcast_to(kept[2:3, :], (8, 128))
    lifted = jnp.broadcast_to(upper[count - 1, pl.ds(TOP, 8), :][0:1, SPARE : SPARE + 1], (8, 128))
    factor = jnp.where(is_final, down, lifted)
    for ref in (one, two):
        zero_spare(ref, 1, rows)
    sources = [upper, one.at[0], two.at[0]]
    targets = [one.at[0], two.at[0], None]
    for step, (d0, d1) in enumerate(steps):
        level = FS - 1 - step

        def move(row, step=step, d0=d0, d1=d1, level=level, keep=True):
            window = pl.ds(row, 8)
            for c, value in enumerate(lap_rows(sources[step], held.at[0], held.at[1], row)):
                value = d0 * sources[step][c, window, :] + d1 * value + held[3 + step, c, window, :]
                if targets[step] is not None:
                    targets[step][c, window, :] = value
                if keep and c < own:
                    to_row, lanes = pl.ds(pl.multiple_of(row - TOP, 8), 8), pl.ds(128 * c, 128)
                    out[level, to_row, lanes] = value
                    if step == 0:
                        out[0, to_row, lanes] = factor * upper[c, window, :] + offset[c, window, :]

        row_loop(TOP, TOP + own_rows, move)
        if targets[step] is not None:
            for row in (8, TOP + own_rows):
                move(row, keep=False)


def chain_kernel(upper, held, offset, factor, here, sums):
    rows, count = held.shape[2], held.shape[1]
    zero = jnp.zeros((8, 128), jnp.float32)
    for c in range(count):
        for row in (0, rows - 8):
            here[c, pl.ds(row, 8), :] = zero

    def move(row):
        for c in range(count):
            window = pl.ds(row, 8)
            here[c, window, :] = factor[...] * upper[c, window, :] + offset[c, window, :]

    row_loop(8, rows - 8, move)

    def body(i, carry):
        row = pl.multiple_of(i * 8, 8)
        image = lap_rows(here, held.at[0], held.at[1], row)
        plain, curved = carry
        for c in range(count - 1):
            value = here[c, pl.ds(row, 8), :]
            plain, curved = plain + value * value, curved + value * image[c]
        return plain, curved

    plain, curved = lax.fori_loop(TOP // 8, (rows - TOP) // 8, body, (zero, zero))
    sums[0], sums[1] = plain, curved


def call(kernel, outs, scratch, args, name):
    return pl.pallas_call(
        kernel,
        out_shape=tuple(jax.ShapeDtypeStruct(shape, jnp.float32) for shape in outs),
        in_specs=[pl.BlockSpec(memory_space=pltpu.VMEM)] * len(args),
        out_specs=tuple(pl.BlockSpec(memory_space=pltpu.VMEM) for _ in outs),
        scratch_shapes=[pltpu.VMEM(shape, jnp.float32) for shape in scratch],
        name=name,
    )(*args)


def swapped(low, high, axis, ring):
    size = lax.axis_size(axis)
    assert size % 2 == 0
    first = [(i, i ^ 1) for i in range(size)]
    second = []
    for i in range(1, size, 2):
        if ring or i + 1 < size:
            second += [(i, (i + 1) % size), ((i + 1) % size, i)]
    return lax.ppermute(low, axis, first), lax.ppermute(high, axis, second)


def exchanged(block):
    return lax.all_to_all(block, ("lat", "lon"), 0, 0, tiled=True)


def local(forcing, depth, mask, guess):
    rows, cols = depth.shape
    count = cols // 128 + 1
    total = rows + 4 * HALO
    fields = FS + 2
    peers = lax.axis_size("lat") * lax.axis_size("lon")
    field = (count, total, 128)

    lat_odd = lax.axis_index("lat") % 2 == 1
    sea = jnp.where(mask > 0, depth, 0.0)
    ordered = [sea, guess[0]] + [forcing[level] for level in range(FS - 1, -1, -1)]
    upper_edge = jnp.concatenate([x[:HALO] for x in ordered])
    lower_edge = jnp.concatenate([x[-HALO:] for x in ordered])
    low, high = swapped(
        jnp.where(lat_odd, upper_edge, lower_edge), jnp.where(lat_odd, lower_edge, upper_edge), "lat", False
    )
    vectors = -(-fields * (rows // 8 + 2) // 16)
    packs = call(
        functools.partial(pack_kernel, fields),
        [(8 * vectors, 128)] * 2,
        [],
        (depth, mask, forcing, guess, low, high),
        "pack",
    )
    low_col, high_col = swapped(*packs, "lon", True)
    held, extra, sums = call(
        relax_kernel,
        [(fields + 1,) + field, (len(EXTRA), count - 1, rows, 128), (peers, 8, 128)],
        [((FS + 1) * (FS + 4) // 2,) + field, field, (1024, 128)],
        (depth, mask, forcing, guess, low, high, low_col, high_col),
        "relax",
    )
    here, offset, kept = call(
        slab_kernel, [field, field, (8, 128)], [(1,) + field] * 2, (exchanged(sums), held), "slab"
    )
    slabs = lax.axis_size("tm")
    back = [(i, i - 1) for i in range(1, slabs)]
    moved = lax.ppermute(here, "tm", back)
    is_final = lax.axis_index("tm") == slabs - 1
    spare_place = (count - 1, TOP, SPARE)
    for _ in range(slabs - 2):
        factor = jnp.where(is_final, kept[2, 0], moved[spare_place])
        upper = jnp.where(is_final, held[2], moved)
        here, parts = call(
            chain_kernel,
            [field, (2, 8, 128)],
            [],
            (upper, held, offset, jnp.full((8, 128), factor)),
            "chain",
        )
        norm, curve = lax.psum((jnp.sum(parts[0]), jnp.sum(parts[1])), ("lat", "lon"))
        here = here.at[count - 1, :, SPARE].set(norm / (norm + FS * curve + EPSILON))
        moved = lax.ppermute(here, "tm", back)
    upper, sums = call(
        moment_kernel,
        [field, (peers, 8, 128)],
        [(FS + 1,) + field, (1024, 128)],
        (moved, held, extra),
        "moment",
    )
    (out,) = call(
        correct_kernel,
        [(FS, rows, cols)],
        [(1,) + field] * 2,
        (exchanged(sums), kept, upper, held, offset),
        "correct",
    )
    return out


def solution(mesh):
    return jax.shard_map(
        local,
        mesh=mesh,
        in_specs=(P("tm", "lat", "lon"), P("lat", "lon"), P("lat", "lon"), P("tm", "lat", "lon")),
        out_specs=P("tm", "lat", "lon"),
        check_vma=False,
    )
```

```python
import functools
import math
import jax
import jax.numpy as jnp
from jax import lax
from jax.experimental import pallas as pl
from jax.experimental.pallas import tpu as pltpu
from jax.sharding import PartitionSpec as P

FS = 4
COUPLING = 3.0
EPSILON = 1e-06
HALO = 8
TOP = 2 * HALO

LENGTHS_RELAX = {
    (i, j): (2 * (FS + 1) - i - j if i or j else 2 * FS + 2) for i in range(FS + 1) for j in range(i, FS + 1)
}
LENGTHS_CORRECT = {(0, j): 2 * FS - j for j in range(FS - 1)}
SPARE_BYTES = 2 << 20
SPARE = 64


def offsets_of(lengths):
    places, at = {}, 0
    for pair, length in lengths.items():
        places[pair] = at
        at += length
    return places


PLACES_RELAX = offsets_of(LENGTHS_RELAX)
PLACES_CORRECT = offsets_of(LENGTHS_CORRECT)


def two_sum(a, b):
    s = a + b
    t = s - a
    return s, (a - (s - t)) + (b - t)


def quick_sum(a, b):
    s = a + b
    return s, b - (s - a)


def pair_add(x, y):
    s, e = two_sum(x[0], y[0])
    return quick_sum(s, e + (x[1] + y[1]))


def split(a):
    t = 4097.0 * a
    hi = t - (t - a)
    return hi, a - hi


def pair_scale(x, d):
    p = x[0] * d
    ah, al = split(x[0])
    bh, bl = split(d)
    e = ((ah * bh - p) + ah * bl + al * bh) + al * bl
    return quick_sum(p, e + x[1] * d)


def tree(items):
    while len(items) > 1:
        items = [pair_add(items[i], items[i + 1]) if i + 1 < len(items) else items[i] for i in range(0, len(items), 2)]
    return items[0]


def roll_pair(x, shift, axis):
    return tuple(pltpu.roll(part, shift, axis) for part in x)


def spread_first(x):
    return jnp.broadcast_to(x[0:1, 0:1], (8, 128))


def lap_rows(src, east, north, row):
    count = east.shape[0]
    lane = lax.broadcasted_iota(jnp.int32, (8, 128), 1)
    last, first = lane == 127, lane == 0
    v = [src[c, pl.ds(row, 8), :] for c in range(count)]
    turned = [pltpu.roll(x, 127, 1) for x in v]
    flux = [
        east[c, pl.ds(row, 8), :] * (v[c] - jnp.where(last, turned[(c + 1) % count], turned[c])) for c in range(count)
    ]
    back = [pltpu.roll(x, 1, 1) for x in flux]
    out = []
    for c in range(count):
        below = north[c, pl.ds(row, 8), :] * (v[c] - src[c, pl.ds(row + 1, 8), :])
        above = north[c, pl.ds(row - 1, 8), :] * (src[c, pl.ds(row - 1, 8), :] - v[c])
        out.append(flux[c] - jnp.where(first, back[(c - 1) % count], back[c]) + below - above)
    return out


def row_loop(start, stop, body):
    def turn(i, carry):
        body(pl.multiple_of(i * 8, 8))
        return carry

    lax.fori_loop(start // 8, stop // 8, turn, 0)


def zero_spare(ref, lead, rows):
    for k in range(lead):
        for c in range(ref.shape[1]):
            ref[k, c, pl.ds(0, 8), :] = jnp.zeros((8, 128), jnp.float32)
            ref[k, c, pl.ds(rows - 8, 8), :] = jnp.zeros((8, 128), jnp.float32)


def dot_groups(acc, groups, load, rows, tiles):
    for group in groups:
        keys = sorted({k for _, a, b in group for k in (a, b)})

        def body(i, carry):
            row = pl.multiple_of(i * 8, 8)
            for c in range(tiles):
                held = {k: load(k, c, row) for k in keys}
                carry = tuple(old + held[a] * held[b] for old, (_, a, b) in zip(carry, group))
            return carry

        sums = lax.fori_loop(
            0, rows // 8, body, tuple(jnp.zeros((8, 128), jnp.float32) for _ in group)
        )
        for total, (m, _, _) in zip(sums, group):
            acc[pl.ds(8 * m, 8), :] = total


def reduce_acc(acc, count, out_ref):
    zero = jnp.zeros((128, 128), jnp.float32)
    for m in range(count, 128):
        acc[pl.ds(8 * m, 8), :] = jnp.zeros((8, 128), jnp.float32)
    hi, lo = tree([(acc[pl.ds(s, 128, stride=8), :], zero) for s in range(8)])
    hi, lo = hi.T, lo.T
    both = tree([(hi[8 * k : 8 * k + 8], lo[8 * k : 8 * k + 8]) for k in range(16)])
    for shift in (4, 2, 1):
        both = pair_add(both, roll_pair(both, shift, 0))
    sub = lax.broadcasted_iota(jnp.int32, (8, 128), 0)
    block = jnp.where(sub == 0, both[0], jnp.where(sub == 1, both[1], 0.0))
    for k in range(out_ref.shape[0]):
        out_ref[k] = block


def gather_sum(ref):
    rows = [(ref[k, 0:1, :], ref[k, 1:2, :]) for k in range(ref.shape[0])]
    hi, lo = tree(rows)
    return jnp.broadcast_to(hi, (8, 128)), jnp.broadcast_to(lo, (8, 128))


def rows_of(moments, places):
    sub = lax.broadcasted_iota(jnp.int32, (8, 128), 0)
    out = []
    for part in moments:
        built = jnp.zeros((8, 128), jnp.float32)
        for row, at in places.items():
            moved = pltpu.roll(part, (128 - at) % 128, 1) if at else part
            built = jnp.where(sub == row, moved, built)
        out.append(built)
    return tuple(out)


def fine_factors(n0, n1, n2, n3):
    den = n0 + n1 + EPSILON
    a0 = n0 / den
    left = (n1 + EPSILON) / den
    s1 = jnp.maximum(left * left * n0 - 2.0 * left * a0 * n1 + a0 * a0 * n2, 0.0)
    big = left + s1 / (n0 + EPSILON)
    small = -a0
    curve = big * big * (n0 + n1) + 2.0 * big * small * (n1 + n2) + small * small * (n2 + n3)
    a1 = jnp.clip(s1 / (curve + EPSILON), 0.0, 1.0)
    return a0 + a1 * big, a1 * small


def coarse_factor(state):
    n0 = state[0]
    n1 = pltpu.roll(n0, 127, 1)
    return spread_first(n0 / (n0 + FS * n1 + EPSILON))


def factors_of(state):
    n0 = state[0]
    d0, d1 = fine_factors(n0, pltpu.roll(n0, 127, 1), pltpu.roll(n0, 126, 1), pltpu.roll(n0, 125, 1))
    return spread_first(d0), spread_first(d1)


def advance(state, gram, step, factors):
    d0, d1 = factors
    sub = lax.broadcasted_iota(jnp.int32, (8, 128), 0)

    def mixed(x, plus):
        moved = pair_add(pair_scale(x, d0), pair_scale(roll_pair(x, 127, 1), d1))
        return pair_add(moved, plus)

    def row(x, r):
        return tuple(jnp.broadcast_to(part[r : r + 1, :], (8, 128)) for part in x)

    cross = row(state, step)
    plus = tuple(jnp.where(sub == 0, a, b) for a, b in zip(cross, gram))
    half = mixed(state, plus)
    full = mixed(half, row(half, step))
    return tuple(jnp.where(sub == 0, a, b) for a, b in zip(full, half))


def gram_rows(moments, step, last):
    return rows_of(moments, {h: PLACES_RELAX[step, h] for h in range(step, last + 1)})


def pack_kernel(fields, depth, mask, forcing, guess, low_in, high_in, low_out, high_out):
    lat_odd = lax.rem(lax.axis_index("lat"), 2) == 1
    lon_odd = lax.rem(lax.axis_index("lon"), 2) == 1
    rows, cols = depth.shape
    tiles = rows // 8 + 2
    lane = lax.broadcasted_iota(jnp.int32, (8, 128), 1) // 8
    edges = []
    for start in (cols - 128, 0):
        window = pl.ds(start, 128)

        def tile(f, t):
            if t in (0, tiles - 1):
                a, b = low_in[pl.ds(8 * f, 8), window], high_in[pl.ds(8 * f, 8), window]
                return jnp.where(lat_odd, a, b) if t == 0 else jnp.where(lat_odd, b, a)
            own = pl.ds(8 * (t - 1), 8)
            if f == 0:
                return jnp.where(mask[own, window] > 0, depth[own, window], 0.0)
            if f == 1:
                return guess[0, own, window]
            return forcing[FS + 1 - f, own, window]

        packed = [jnp.zeros((8, 128), jnp.float32) for _ in range(-(-fields * tiles // 16))]
        for f in range(fields):
            for t in range(tiles):
                at, slot = divmod(f * tiles + t, 16)
                shift = (8 * slot + (8 if start else 0)) % 128
                value = tile(f, t)
                value = pltpu.roll(value, shift, 1) if shift else value
                packed[at] = jnp.where(lane == slot, value, packed[at])
        edges.append(packed)
    for k, (e, w) in enumerate(zip(*edges)):
        low_out[pl.ds(8 * k, 8), :] = jnp.where(lon_odd, w, e)
        high_out[pl.ds(8 * k, 8), :] = jnp.where(lon_odd, e, w)


def relax_kernel(depth, mask, forcing, guess, low_in, high_in, low_col, high_col, held, extra, sums, kry, wet, acc):
    lat_odd = lax.rem(lax.axis_index("lat"), 2) == 1
    lon_odd = lax.rem(lax.axis_index("lon"), 2) == 1
    rows, cols = depth.shape
    own = cols // 128
    count = own + 1
    tiles = rows // 8 + 2
    total = rows + 4 * HALO
    lane = lax.broadcasted_iota(jnp.int32, (8, 128), 1)
    fields = FS + 2
    zero = jnp.zeros((8, 128), jnp.float32)

    def put(f, c, row, value):
        if f == 0:
            wet[c, pl.ds(row, 8), :] = value
        else:
            kry[start_of[f - 1], c, pl.ds(row, 8), :] = value
            held[1 + f, c, pl.ds(row, 8), :] = value

    start_of, at = {}, 0
    for s in range(FS + 1):
        start_of[s] = at
        at += FS + 2 - s
    zero_spare(kry, at, total)
    for c in range(count):
        for row in (0, total - 8):
            wet[c, pl.ds(row, 8), :] = zero
            for k in range(fields + 1):
                held[k, c, pl.ds(row, 8), :] = zero
    for f in range(fields):
        for c in range(own):
            window = pl.ds(128 * c, 128)
            a, b = low_in[pl.ds(8 * f, 8), window], high_in[pl.ds(8 * f, 8), window]
            put(f, c, TOP - 8, jnp.where(lat_odd, a, b))
            put(f, c, TOP + rows, jnp.where(lat_odd, b, a))
        for t in range(tiles):
            k, slot = divmod(f * tiles + t, 16)
            a, b = low_col[pl.ds(8 * k, 8), :], high_col[pl.ds(8 * k, 8), :]
            e, w = jnp.where(lon_odd, b, a), jnp.where(lon_odd, a, b)
            e = pltpu.roll(e, 128 - 8 * slot, 1) if slot else e
            w = pltpu.roll(w, (120 - 8 * slot) % 128, 1) if slot < 15 else w
            put(f, own, TOP - 8 + 8 * t, jnp.where(lane < 8, e, jnp.where(lane >= 120, w, 0.0)))

    def fill(row):
        from_row = pl.ds(pl.multiple_of(row - TOP, 8), 8)
        for c in range(own):
            window = pl.ds(128 * c, 128)
            put(0, c, row, jnp.where(mask[from_row, window] > 0, depth[from_row, window], 0.0))
            put(1, c, row, guess[0, from_row, window])
            for f in range(2, fields):
                put(f, c, row, forcing[FS + 1 - f, from_row, window])

    row_loop(TOP, TOP + rows, fill)

    def faces(row):
        d = [wet[c, pl.ds(row, 8), :] for c in range(count)]
        turned = [pltpu.roll(x, 127, 1) for x in d]
        for c in range(count):
            right = jnp.where(lane == 127, turned[(c + 1) % count], turned[c])
            under = wet[c, pl.ds(row + 1, 8), :]
            half = COUPLING * 0.5
            held[0, c, pl.ds(row, 8), :] = jnp.where((d[c] > 0) & (right > 0), half * (d[c] + right), 0.0)
            held[1, c, pl.ds(row, 8), :] = jnp.where((d[c] > 0) & (under > 0), half * (d[c] + under), 0.0)

    row_loop(8, total - 8, faces)
    east, north = held.at[0], held.at[1]

    for degree in range(FS + 1):
        def power(row, degree=degree):
            for s in range(FS + 1 - degree):
                at = start_of[s] + degree
                for c, value in enumerate(lap_rows(kry.at[at], east, north, row)):
                    kry[at + 1, c, pl.ds(row, 8), :] = value

        row_loop(8, total - 8, power)

    def copy(row):
        to_row = pl.ds(pl.multiple_of(row - TOP, 8), 8)
        for k, (s, degree) in enumerate(EXTRA):
            for c in range(own):
                extra[k, c, to_row, :] = kry[start_of[s] + degree, c, pl.ds(row, 8), :]

    row_loop(TOP, TOP + rows, copy)

    groups, group = [], []
    for (i, j), length in LENGTHS_RELAX.items():
        if len(group) + length > 26:
            groups.append(group)
            group = []
        for k in range(length):
            b = min(k // 2, FS + 1 - j)
            group.append((PLACES_RELAX[i, j] + k, start_of[i] + k - b, start_of[j] + b))
    groups.append(group)
    dot_groups(acc, groups, lambda k, c, row: kry[k, c, pl.ds(row + TOP, 8), :], rows, own)
    reduce_acc(acc, sum(LENGTHS_RELAX.values()), sums)


EXTRA = ((1, 1), (1, 2), (2, 1))


def slab_kernel(gathered, held, here, offset, kept, one, two):
    rows = held.shape[2]
    count = held.shape[1]
    lane = lax.broadcasted_iota(jnp.int32, (8, 128), 1)
    sub = lax.broadcasted_iota(jnp.int32, (8, 128), 0)
    moments = gather_sum(gathered)
    state = rows_of(moments, {j: PLACES_RELAX[0, j] for j in range(FS + 1)})
    down = coarse_factor(state)
    steps = []
    for step in range(1, FS + 1):
        factors = factors_of(state)
        steps.append(factors)
        state = advance(state, gram_rows(moments, step, FS), step, factors)
    sent = coarse_factor(state)
    kept[...] = jnp.where(sub == 0, moments[0], jnp.where(sub == 1, moments[1], jnp.where(sub == 2, down, 0.0)))
    east, north = held.at[0], held.at[1]
    for ref in (one, two):
        zero_spare(ref, 1, rows)
    zero = jnp.zeros((8, 128), jnp.float32)
    for c in range(count):
        for row in (0, rows - 8):
            here[c, pl.ds(row, 8), :] = zero
            offset[c, pl.ds(row, 8), :] = zero
    sources = [held.at[2], one.at[0], two.at[0], one.at[0]]
    targets = [one.at[0], two.at[0], one.at[0], None]
    for step, (d0, d1) in enumerate(steps):
        def move(row, step=step, d0=d0, d1=d1):
            for c, value in enumerate(lap_rows(sources[step], east, north, row)):
                window = pl.ds(row, 8)
                value = d0 * sources[step][c, window, :] + d1 * value + held[3 + step, c, window, :]
                if targets[step] is not None:
                    targets[step][c, window, :] = value
                else:
                    coarse = down * held[2, c, window, :]
                    rest = value - coarse
                    offset[c, window, :] = rest
                    value = coarse + rest
                    if c == count - 1:
                        value = jnp.where(lane == SPARE, sent, value)
                    here[c, window, :] = value

        row_loop(8, rows - 8, move)


def moment_kernel(moved, held, extra, upper, sums, kry, acc):
    is_final = lax.axis_index("tm") == lax.axis_size("tm") - 1
    rows, count = held.shape[2], held.shape[1]
    own_rows, own = extra.shape[2], extra.shape[1]
    zero_spare(kry, FS + 1, rows)
    zero = jnp.zeros((8, 128), jnp.float32)
    for c in range(count):
        for row in (0, rows - 8):
            upper[c, pl.ds(row, 8), :] = zero

    def choose(row):
        for c in range(count):
            window = pl.ds(row, 8)
            value = jnp.where(is_final, held[2, c, window, :], moved[c, window, :])
            upper[c, window, :] = value
            kry[0, c, window, :] = value

    row_loop(8, rows - 8, choose)
    for degree in range(FS):
        def power(row, degree=degree):
            for c, value in enumerate(lap_rows(kry.at[degree], held.at[0], held.at[1], row)):
                kry[degree + 1, c, pl.ds(row, 8), :] = value

        row_loop(8, rows - 8, power)

    def load(key, c, row):
        s, degree = key
        if s == 0:
            return kry[degree, c, pl.ds(row + TOP, 8), :]
        if degree == 0:
            return held[2 + s, c, pl.ds(row + TOP, 8), :]
        return extra[EXTRA.index(key), c, pl.ds(row, 8), :]

    group = []
    for (i, j), length in LENGTHS_CORRECT.items():
        for k in range(length):
            b = max(k - FS, 0) if j else k // 2
            group.append((PLACES_CORRECT[i, j] + k, (0, k - b), (j, b)))
    dot_groups(acc, [group], load, own_rows, own)
    reduce_acc(acc, sum(LENGTHS_CORRECT.values()), sums)


def correct_kernel(gathered, kept, upper, held, offset, out, one, two):
    is_final = lax.axis_index("tm") == lax.axis_size("tm") - 1
    rows, count = held.shape[2], held.shape[1]
    own_rows, own = out.shape[1], out.shape[2] // 128
    moments = gather_sum(gathered)
    before = tuple(jnp.broadcast_to(kept[k : k + 1, :], (8, 128)) for k in range(2))
    state = rows_of(moments, {j: PLACES_CORRECT[0, j] for j in range(FS - 1)})
    steps = []
    for step in range(1, FS):
        factors = factors_of(state)
        steps.append(factors)
        if step < FS - 1:
            state = advance(state, gram_rows(before, step, FS - 2), step, factors)
    down = jnp.broadcast_to(kept[2:3, :], (8, 128))
    lifted = jnp.broadcast_to(upper[count - 1, pl.ds(TOP, 8), :][0:1, SPARE : SPARE + 1], (8, 128))
    factor = jnp.where(is_final, down, lifted)
    for ref in (one, two):
        zero_spare(ref, 1, rows)
    sources = [upper, one.at[0], two.at[0]]
    targets = [one.at[0], two.at[0], None]
    for step, (d0, d1) in enumerate(steps):
        level = FS - 1 - step

        def move(row, step=step, d0=d0, d1=d1, level=level, keep=True):
            window = pl.ds(row, 8)
            for c, value in enumerate(lap_rows(sources[step], held.at[0], held.at[1], row)):
                value = d0 * sources[step][c, window, :] + d1 * value + held[3 + step, c, window, :]
                if targets[step] is not None:
                    targets[step][c, window, :] = value
                if keep and c < own:
                    to_row, lanes = pl.ds(pl.multiple_of(row - TOP, 8), 8), pl.ds(128 * c, 128)
                    out[level, to_row, lanes] = value
                    if step == 0:
                        out[0, to_row, lanes] = factor * upper[c, window, :] + offset[c, window, :]

        row_loop(TOP, TOP + own_rows, move)
        if targets[step] is not None:
            for row in (8, TOP + own_rows):
                move(row, keep=False)


def chain_kernel(upper, held, offset, factor, here, sums):
    rows, count = held.shape[2], held.shape[1]
    zero = jnp.zeros((8, 128), jnp.float32)
    for c in range(count):
        for row in (0, rows - 8):
            here[c, pl.ds(row, 8), :] = zero

    def move(row):
        for c in range(count):
            window = pl.ds(row, 8)
            here[c, window, :] = factor[...] * upper[c, window, :] + offset[c, window, :]

    row_loop(8, rows - 8, move)

    def body(i, carry):
        row = pl.multiple_of(i * 8, 8)
        image = lap_rows(here, held.at[0], held.at[1], row)
        plain, curved = carry
        for c in range(count - 1):
            value = here[c, pl.ds(row, 8), :]
            plain, curved = plain + value * value, curved + value * image[c]
        return plain, curved

    plain, curved = lax.fori_loop(TOP // 8, (rows - TOP) // 8, body, (zero, zero))
    sums[0], sums[1] = plain, curved


def call(kernel, outs, scratch, args, name):
    held = sum(math.prod(shape) * 4 for shape in (*outs, *scratch, *(x.shape for x in args)))
    return pl.pallas_call(
        kernel,
        out_shape=tuple(jax.ShapeDtypeStruct(shape, jnp.float32) for shape in outs),
        in_specs=[pl.BlockSpec(memory_space=pltpu.VMEM)] * len(args),
        out_specs=tuple(pl.BlockSpec(memory_space=pltpu.VMEM) for _ in outs),
        scratch_shapes=[pltpu.VMEM(shape, jnp.float32) for shape in scratch],
        compiler_params=pltpu.CompilerParams(vmem_limit_bytes=held + SPARE_BYTES),
        name=name,
    )(*args)


def swapped(low, high, axis, ring):
    size = lax.axis_size(axis)
    assert size % 2 == 0
    first = [(i, i ^ 1) for i in range(size)]
    second = []
    for i in range(1, size, 2):
        if ring or i + 1 < size:
            second += [(i, (i + 1) % size), ((i + 1) % size, i)]
    return lax.ppermute(low, axis, first), lax.ppermute(high, axis, second)


def exchanged(block):
    return lax.all_to_all(block, ("lat", "lon"), 0, 0, tiled=True)


def local(forcing, depth, mask, guess):
    rows, cols = depth.shape
    count = cols // 128 + 1
    total = rows + 4 * HALO
    fields = FS + 2
    peers = lax.axis_size("lat") * lax.axis_size("lon")
    field = (count, total, 128)

    lat_odd = lax.axis_index("lat") % 2 == 1
    sea = jnp.where(mask > 0, depth, 0.0)
    ordered = [sea, guess[0]] + [forcing[level] for level in range(FS - 1, -1, -1)]
    upper_edge = jnp.concatenate([x[:HALO] for x in ordered])
    lower_edge = jnp.concatenate([x[-HALO:] for x in ordered])
    low, high = swapped(
        jnp.where(lat_odd, upper_edge, lower_edge), jnp.where(lat_odd, lower_edge, upper_edge), "lat", False
    )
    vectors = -(-fields * (rows // 8 + 2) // 16)
    packs = call(
        functools.partial(pack_kernel, fields),
        [(8 * vectors, 128)] * 2,
        [],
        (depth, mask, forcing, guess, low, high),
        "pack",
    )
    low_col, high_col = swapped(*packs, "lon", True)
    held, extra, sums = call(
        relax_kernel,
        [(fields + 1,) + field, (len(EXTRA), count - 1, rows, 128), (peers, 8, 128)],
        [((FS + 1) * (FS + 4) // 2,) + field, field, (1024, 128)],
        (depth, mask, forcing, guess, low, high, low_col, high_col),
        "relax",
    )
    here, offset, kept = call(
        slab_kernel, [field, field, (8, 128)], [(1,) + field] * 2, (exchanged(sums), held), "slab"
    )
    slabs = lax.axis_size("tm")
    back = [(i, i - 1) for i in range(1, slabs)]
    moved = lax.ppermute(here, "tm", back)
    is_final = lax.axis_index("tm") == slabs - 1
    spare_place = (count - 1, TOP, SPARE)
    for _ in range(slabs - 2):
        factor = jnp.where(is_final, kept[2, 0], moved[spare_place])
        upper = jnp.where(is_final, held[2], moved)
        here, parts = call(
            chain_kernel,
            [field, (2, 8, 128)],
            [],
            (upper, held, offset, jnp.full((8, 128), factor)),
            "chain",
        )
        norm, curve = lax.psum((jnp.sum(parts[0]), jnp.sum(parts[1])), ("lat", "lon"))
        here = here.at[count - 1, :, SPARE].set(norm / (norm + FS * curve + EPSILON))
        moved = lax.ppermute(here, "tm", back)
    upper, sums = call(
        moment_kernel,
        [field, (peers, 8, 128)],
        [(FS + 1,) + field, (1024, 128)],
        (moved, held, extra),
        "moment",
    )
    (out,) = call(
        correct_kernel,
        [(FS, rows, cols)],
        [(1,) + field] * 2,
        (exchanged(sums), kept, upper, held, offset),
        "correct",
    )
    return out


def solution(mesh):
    return jax.shard_map(
        local,
        mesh=mesh,
        in_specs=(P("tm", "lat", "lon"), P("lat", "lon"), P("lat", "lon"), P("tm", "lat", "lon")),
        out_specs=P("tm", "lat", "lon"),
        check_vma=False,
    )
```

```python
import functools
import math
import jax
import jax.numpy as jnp
from jax import lax
from jax.experimental import pallas as pl
from jax.experimental.pallas import tpu as pltpu
from jax.sharding import PartitionSpec as P

FS = 4
COUPLING = 3.0
EPSILON = 1e-06
HALO = 8
TOP = 2 * HALO

LENGTHS_RELAX = {
    (i, j): (2 * (FS + 1) - i - j if i or j else 2 * FS + 2) for i in range(FS + 1) for j in range(i, FS + 1)
}
LENGTHS_CORRECT = {(0, j): 2 * FS - j for j in range(FS - 1)}
SPARE_BYTES = 2 << 20
SPARE = 64


def offsets_of(lengths):
    places, at = {}, 0
    for pair, length in lengths.items():
        places[pair] = at
        at += length
    return places


PLACES_RELAX = offsets_of(LENGTHS_RELAX)
PLACES_CORRECT = offsets_of(LENGTHS_CORRECT)


def two_sum(a, b):
    s = a + b
    t = s - a
    return s, (a - (s - t)) + (b - t)


def quick_sum(a, b):
    s = a + b
    return s, b - (s - a)


def pair_add(x, y):
    s, e = two_sum(x[0], y[0])
    return quick_sum(s, e + (x[1] + y[1]))


def split(a):
    t = 4097.0 * a
    hi = t - (t - a)
    return hi, a - hi


def pair_scale(x, d):
    p = x[0] * d
    ah, al = split(x[0])
    bh, bl = split(d)
    e = ((ah * bh - p) + ah * bl + al * bh) + al * bl
    return quick_sum(p, e + x[1] * d)


def tree(items):
    while len(items) > 1:
        items = [pair_add(items[i], items[i + 1]) if i + 1 < len(items) else items[i] for i in range(0, len(items), 2)]
    return items[0]


def roll_pair(x, shift, axis):
    return tuple(pltpu.roll(part, shift, axis) for part in x)


def spread_first(x):
    return jnp.broadcast_to(x[0:1, 0:1], (8, 128))


EAST, WEST, NORTH, START = 0, 1, 2, 3


def lap_rows(src, held, row, tiles):
    count = held.shape[1]
    lane = lax.broadcasted_iota(jnp.int32, (8, 128), 1)
    last, first = lane == 127, lane == 0
    here, below, above = pl.ds(row, 8), pl.ds(row + 1, 8), pl.ds(row - 1, 8)
    v = [src[c, here, :] for c in range(count)]
    left = [pltpu.roll(x, 1, 1) for x in v]
    right = [pltpu.roll(x, 127, 1) for x in v]
    out = []
    for c in range(tiles):
        e = held[EAST, c, here, :] * (v[c] - jnp.where(last, right[(c + 1) % count], right[c]))
        w = held[WEST, c, here, :] * (v[c] - jnp.where(first, left[(c - 1) % count], left[c]))
        n = held[NORTH, c, here, :] * (v[c] - src[c, below, :])
        s = held[NORTH, c, above, :] * (v[c] - src[c, above, :])
        out.append((e + w) + (n + s))
    return out


def zero_spare(ref, lead, rows):
    for k in range(lead):
        for c in range(ref.shape[1]):
            ref[k, c, pl.ds(0, 8), :] = jnp.zeros((8, 128), jnp.float32)
            ref[k, c, pl.ds(rows - 8, 8), :] = jnp.zeros((8, 128), jnp.float32)


def dot_groups(acc, groups, load, rows, tiles):
    for group in groups:
        keys = sorted({k for _, a, b in group for k in (a, b)})

        def body(i, carry):
            row = pl.multiple_of(i * 8, 8)
            for c in range(tiles):
                held = {k: load(k, c, row) for k in keys}
                carry = tuple(old + held[a] * held[b] for old, (_, a, b) in zip(carry, group))
            return carry

        sums = lax.fori_loop(
            0, rows // 8, body, tuple(jnp.zeros((8, 128), jnp.float32) for _ in group)
        )
        for total, (m, _, _) in zip(sums, group):
            acc[pl.ds(8 * m, 8), :] = total


def reduce_acc(acc, count, out_ref):
    zero = jnp.zeros((128, 128), jnp.float32)
    for m in range(count, 128):
        acc[pl.ds(8 * m, 8), :] = jnp.zeros((8, 128), jnp.float32)
    hi, lo = tree([(acc[pl.ds(s, 128, stride=8), :], zero) for s in range(8)])
    hi, lo = hi.T, lo.T
    both = tree([(hi[8 * k : 8 * k + 8], lo[8 * k : 8 * k + 8]) for k in range(16)])
    for shift in (4, 2, 1):
        both = pair_add(both, roll_pair(both, shift, 0))
    sub = lax.broadcasted_iota(jnp.int32, (8, 128), 0)
    block = jnp.where(sub == 0, both[0], jnp.where(sub == 1, both[1], 0.0))
    for k in range(out_ref.shape[0]):
        out_ref[k] = block


def gather_sum(ref):
    rows = [(ref[k, 0:1, :], ref[k, 1:2, :]) for k in range(ref.shape[0])]
    hi, lo = tree(rows)
    return jnp.broadcast_to(hi, (8, 128)), jnp.broadcast_to(lo, (8, 128))


def rows_of(moments, places):
    sub = lax.broadcasted_iota(jnp.int32, (8, 128), 0)
    out = []
    for part in moments:
        built = jnp.zeros((8, 128), jnp.float32)
        for row, at in places.items():
            moved = pltpu.roll(part, (128 - at) % 128, 1) if at else part
            built = jnp.where(sub == row, moved, built)
        out.append(built)
    return tuple(out)


def fine_factors(n0, n1, n2, n3):
    den = n0 + n1 + EPSILON
    a0 = n0 / den
    left = (n1 + EPSILON) / den
    s1 = jnp.maximum(left * left * n0 - 2.0 * left * a0 * n1 + a0 * a0 * n2, 0.0)
    big = left + s1 / (n0 + EPSILON)
    small = -a0
    curve = big * big * (n0 + n1) + 2.0 * big * small * (n1 + n2) + small * small * (n2 + n3)
    a1 = jnp.clip(s1 / (curve + EPSILON), 0.0, 1.0)
    return a0 + a1 * big, a1 * small


def coarse_factor(state):
    n0 = state[0]
    n1 = pltpu.roll(n0, 127, 1)
    return spread_first(n0 / (n0 + FS * n1 + EPSILON))


def factors_of(state):
    n0 = state[0]
    d0, d1 = fine_factors(n0, pltpu.roll(n0, 127, 1), pltpu.roll(n0, 126, 1), pltpu.roll(n0, 125, 1))
    return spread_first(d0), spread_first(d1)


def advance(state, gram, step, factors):
    d0, d1 = factors
    sub = lax.broadcasted_iota(jnp.int32, (8, 128), 0)

    def mixed(x, plus):
        moved = pair_add(pair_scale(x, d0), pair_scale(roll_pair(x, 127, 1), d1))
        return pair_add(moved, plus)

    def row(x, r):
        return tuple(jnp.broadcast_to(part[r : r + 1, :], (8, 128)) for part in x)

    cross = row(state, step)
    plus = tuple(jnp.where(sub == 0, a, b) for a, b in zip(cross, gram))
    half = mixed(state, plus)
    full = mixed(half, row(half, step))
    return tuple(jnp.where(sub == 0, a, b) for a, b in zip(full, half))


def gram_rows(moments, step, last):
    return rows_of(moments, {h: PLACES_RELAX[step, h] for h in range(step, last + 1)})


def tile_kernel(depth, mask, forcing, guess, own, low, high):
    odd = lax.rem(lax.axis_index("lat"), 2) == 1
    rows = depth.shape[0]
    for c in range(own.shape[1]):
        window = pl.ds(128 * c, 128)
        own[0, c] = jnp.where(mask[:, window] > 0, depth[:, window], 0.0)
        own[1, c] = guess[0, :, window]
        for f in range(2, FS + 2):
            own[f, c] = forcing[FS + 1 - f, :, window]
        for f in range(FS + 2):
            a, b = own[f, c, pl.ds(0, 8), :], own[f, c, pl.ds(rows - 8, 8), :]
            low[pl.ds(8 * f, 8), window] = jnp.where(odd, a, b)
            high[pl.ds(8 * f, 8), window] = jnp.where(odd, b, a)


def pack_kernel(own, low_in, high_in, low_out, high_out):
    lat_odd = lax.rem(lax.axis_index("lat"), 2) == 1
    lon_odd = lax.rem(lax.axis_index("lon"), 2) == 1
    fields, tiles = own.shape[0], own.shape[2] // 8 + 2
    lane = lax.broadcasted_iota(jnp.int32, (8, 128), 1) // 8
    edges = []
    for c in (own.shape[1] - 1, 0):
        window = pl.ds(128 * c, 128)

        def tile(f, t):
            if t in (0, tiles - 1):
                a, b = low_in[pl.ds(8 * f, 8), window], high_in[pl.ds(8 * f, 8), window]
                return jnp.where(lat_odd, a, b) if t == 0 else jnp.where(lat_odd, b, a)
            return own[f, c, pl.ds(8 * (t - 1), 8), :]

        packed = [jnp.zeros((8, 128), jnp.float32) for _ in range(-(-fields * tiles // 16))]
        for f in range(fields):
            for t in range(tiles):
                at, slot = divmod(f * tiles + t, 16)
                shift = (8 * slot + (8 if c else 0)) % 128
                value = tile(f, t)
                value = pltpu.roll(value, shift, 1) if shift else value
                packed[at] = jnp.where(lane == slot, value, packed[at])
        edges.append(packed)
    for k, (e, w) in enumerate(zip(*edges)):
        low_out[pl.ds(8 * k, 8), :] = jnp.where(lon_odd, w, e)
        high_out[pl.ds(8 * k, 8), :] = jnp.where(lon_odd, e, w)


def relax_kernel(own_fields, low_in, high_in, low_col, high_col, held, extra, sums, kry, wet, acc):
    lat_odd = lax.rem(lax.axis_index("lat"), 2) == 1
    lon_odd = lax.rem(lax.axis_index("lon"), 2) == 1
    fields, own, rows, _ = own_fields.shape
    count = own + 1
    tiles = rows // 8 + 2
    total = rows + 4 * HALO
    lane = lax.broadcasted_iota(jnp.int32, (8, 128), 1)
    zero = jnp.zeros((8, 128), jnp.float32)

    def put(f, c, row, value):
        if f == 0:
            wet[c, pl.ds(row, 8), :] = value
        else:
            held[START - 1 + f, c, pl.ds(row, 8), :] = value

    start_of, at = {}, 0
    for s in range(FS + 1):
        start_of[s] = at
        at += FS + 1 - s
    zero_spare(kry, at, total)
    zero_spare(held, held.shape[0], total)
    for c in range(count):
        for row in (0, total - 8):
            wet[c, pl.ds(row, 8), :] = zero
    for f in range(fields):
        for c in range(own):
            window = pl.ds(128 * c, 128)
            a, b = low_in[pl.ds(8 * f, 8), window], high_in[pl.ds(8 * f, 8), window]
            put(f, c, TOP - 8, jnp.where(lat_odd, a, b))
            put(f, c, TOP + rows, jnp.where(lat_odd, b, a))
            for row in range(0, rows, 8):
                put(f, c, TOP + row, own_fields[f, c, pl.ds(row, 8), :])
        for t in range(tiles):
            k, slot = divmod(f * tiles + t, 16)
            a, b = low_col[pl.ds(8 * k, 8), :], high_col[pl.ds(8 * k, 8), :]
            e, w = jnp.where(lon_odd, b, a), jnp.where(lon_odd, a, b)
            e = pltpu.roll(e, 128 - 8 * slot, 1) if slot else e
            w = pltpu.roll(w, (120 - 8 * slot) % 128, 1) if slot < 15 else w
            put(f, own, TOP - 8 + 8 * t, jnp.where(lane < 8, e, jnp.where(lane >= 120, w, 0.0)))

    half = COUPLING * 0.5
    for row in range(8, total - 8, 8):
        d = [wet[c, pl.ds(row, 8), :] for c in range(count)]
        left = [pltpu.roll(x, 1, 1) for x in d]
        right = [pltpu.roll(x, 127, 1) for x in d]
        for c in range(count):
            sides = (
                (EAST, jnp.where(lane == 127, right[(c + 1) % count], right[c])),
                (WEST, jnp.where(lane == 0, left[(c - 1) % count], left[c])),
                (NORTH, wet[c, pl.ds(row + 1, 8), :]),
            )
            for place, other in sides:
                held[place, c, pl.ds(row, 8), :] = jnp.where((d[c] > 0) & (other > 0), half * (d[c] + other), 0.0)

    def source(s, degree):
        return kry.at[start_of[s] + degree - 1] if degree else held.at[START + s]

    for degree in range(FS + 1):
        for s in range(FS + 1 - degree):
            final = s + degree == FS
            src, dst = source(s, degree), source(s, degree + 1)
            for row in range(TOP, TOP + rows, 8) if final else range(8, total - 8, 8):
                for c, value in enumerate(lap_rows(src, held, row, own if final else count)):
                    dst[c, pl.ds(row, 8), :] = value

    for k, (s, degree) in enumerate(EXTRA):
        for c in range(own):
            extra[k, c] = source(s, degree)[c, pl.ds(TOP, rows), :]

    groups, group = [], []
    for (i, j), length in LENGTHS_RELAX.items():
        if len(group) + length > 26:
            groups.append(group)
            group = []
        for k in range(length):
            b = min(k // 2, FS + 1 - j)
            group.append((PLACES_RELAX[i, j] + k, (i, k - b), (j, b)))
    groups.append(group)
    dot_groups(acc, groups, lambda key, c, row: source(*key)[c, pl.ds(row + TOP, 8), :], rows, own)
    reduce_acc(acc, sum(LENGTHS_RELAX.values()), sums)


EXTRA = ((1, 1), (1, 2), (2, 1))


def slab_kernel(gathered, held, here, offset, kept, one, two):
    rows = held.shape[2]
    count = held.shape[1]
    lane = lax.broadcasted_iota(jnp.int32, (8, 128), 1)
    sub = lax.broadcasted_iota(jnp.int32, (8, 128), 0)
    moments = gather_sum(gathered)
    state = rows_of(moments, {j: PLACES_RELAX[0, j] for j in range(FS + 1)})
    down = coarse_factor(state)
    steps = []
    for step in range(1, FS + 1):
        factors = factors_of(state)
        steps.append(factors)
        state = advance(state, gram_rows(moments, step, FS), step, factors)
    sent = coarse_factor(state)
    kept[...] = jnp.where(sub == 0, moments[0], jnp.where(sub == 1, moments[1], jnp.where(sub == 2, down, 0.0)))
    for ref in (one, two):
        zero_spare(ref, 1, rows)
    zero = jnp.zeros((8, 128), jnp.float32)
    for c in range(count):
        for row in (0, rows - 8):
            here[c, pl.ds(row, 8), :] = zero
            offset[c, pl.ds(row, 8), :] = zero
    sources = [held.at[START], one.at[0], two.at[0], one.at[0]]
    for step, (d0, d1) in enumerate(steps):
        src = sources[step]
        for row in range(8, rows - 8, 8):
            window = pl.ds(row, 8)
            for c, value in enumerate(lap_rows(src, held, row, count)):
                value = d0 * src[c, window, :] + d1 * value + held[START + 1 + step, c, window, :]
                if step < FS - 1:
                    sources[step + 1][c, window, :] = value
                else:
                    coarse = down * held[START, c, window, :]
                    rest = value - coarse
                    offset[c, window, :] = rest
                    value = coarse + rest
                    if c == count - 1:
                        value = jnp.where(lane == SPARE, sent, value)
                    here[c, window, :] = value


def moment_kernel(moved, held, extra, upper, sums, kry, acc):
    is_final = lax.axis_index("tm") == lax.axis_size("tm") - 1
    rows, count = held.shape[2], held.shape[1]
    own_rows, own = extra.shape[2], extra.shape[1]
    zero_spare(kry, FS, rows)
    zero = jnp.zeros((8, 128), jnp.float32)
    for c in range(count):
        for row in (0, rows - 8):
            upper[c, pl.ds(row, 8), :] = zero

    for row in range(8, rows - 8, 8):
        for c in range(count):
            window = pl.ds(row, 8)
            upper[c, window, :] = jnp.where(is_final, held[START, c, window, :], moved[c, window, :])
    for degree in range(FS):
        final = degree == FS - 1
        src = kry.at[degree - 1] if degree else upper
        for row in range(TOP, TOP + own_rows, 8) if final else range(8, rows - 8, 8):
            for c, value in enumerate(lap_rows(src, held, row, own if final else count)):
                kry[degree, c, pl.ds(row, 8), :] = value

    def load(key, c, row):
        s, degree = key
        if s == 0:
            return (kry.at[degree - 1] if degree else upper)[c, pl.ds(row + TOP, 8), :]
        if degree == 0:
            return held[START + s, c, pl.ds(row + TOP, 8), :]
        return extra[EXTRA.index(key), c, pl.ds(row, 8), :]

    group = []
    for (i, j), length in LENGTHS_CORRECT.items():
        for k in range(length):
            b = max(k - FS, 0) if j else k // 2
            group.append((PLACES_CORRECT[i, j] + k, (0, k - b), (j, b)))
    dot_groups(acc, [group], load, own_rows, own)
    reduce_acc(acc, sum(LENGTHS_CORRECT.values()), sums)


def correct_kernel(gathered, kept, upper, held, offset, out, one, two):
    is_final = lax.axis_index("tm") == lax.axis_size("tm") - 1
    rows, count = held.shape[2], held.shape[1]
    own_rows, own = out.shape[1], out.shape[2] // 128
    moments = gather_sum(gathered)
    before = tuple(jnp.broadcast_to(kept[k : k + 1, :], (8, 128)) for k in range(2))
    state = rows_of(moments, {j: PLACES_CORRECT[0, j] for j in range(FS - 1)})
    steps = []
    for step in range(1, FS):
        factors = factors_of(state)
        steps.append(factors)
        if step < FS - 1:
            state = advance(state, gram_rows(before, step, FS - 2), step, factors)
    down = jnp.broadcast_to(kept[2:3, :], (8, 128))
    lifted = jnp.broadcast_to(upper[count - 1, pl.ds(TOP, 8), :][0:1, SPARE : SPARE + 1], (8, 128))
    factor = jnp.where(is_final, down, lifted)
    for ref in (one, two):
        zero_spare(ref, 1, rows)
    sources = [upper, one.at[0], two.at[0]]
    for step, (d0, d1) in enumerate(steps):
        src, level, final = sources[step], FS - 1 - step, step == FS - 2
        for row in range(TOP, TOP + own_rows, 8) if final else range(8, rows - 8, 8):
            window, to_row = pl.ds(row, 8), pl.ds(row - TOP, 8)
            inside = TOP <= row < TOP + own_rows
            for c, value in enumerate(lap_rows(src, held, row, own if final else count)):
                lanes = pl.ds(128 * c, 128)
                value = d0 * src[c, window, :] + d1 * value + held[START + 1 + step, c, window, :]
                if not final:
                    sources[step + 1][c, window, :] = value
                if inside and c < own:
                    out[level, to_row, lanes] = value
                    if step == 0:
                        out[0, to_row, lanes] = factor * upper[c, window, :] + offset[c, window, :]


def chain_kernel(upper, held, offset, factor, here, sums):
    rows, count = held.shape[2], held.shape[1]
    zero = jnp.zeros((8, 128), jnp.float32)
    for c in range(count):
        for row in (0, rows - 8):
            here[c, pl.ds(row, 8), :] = zero

    for row in range(8, rows - 8, 8):
        for c in range(count):
            window = pl.ds(row, 8)
            here[c, window, :] = factor[...] * upper[c, window, :] + offset[c, window, :]
    plain = curved = zero
    for row in range(TOP, rows - TOP, 8):
        for c, image in enumerate(lap_rows(here, held, row, count - 1)):
            value = here[c, pl.ds(row, 8), :]
            plain, curved = plain + value * value, curved + value * image
    sums[0], sums[1] = plain, curved


def call(kernel, outs, scratch, args, name):
    held = sum(math.prod(shape) * 4 for shape in (*outs, *scratch, *(x.shape for x in args)))
    return pl.pallas_call(
        kernel,
        out_shape=tuple(jax.ShapeDtypeStruct(shape, jnp.float32) for shape in outs),
        in_specs=[pl.BlockSpec(memory_space=pltpu.VMEM)] * len(args),
        out_specs=tuple(pl.BlockSpec(memory_space=pltpu.VMEM) for _ in outs),
        scratch_shapes=[pltpu.VMEM(shape, jnp.float32) for shape in scratch],
        compiler_params=pltpu.CompilerParams(vmem_limit_bytes=held + SPARE_BYTES),
        name=name,
    )(*args)


def swapped(low, high, axis, ring):
    size = lax.axis_size(axis)
    assert size % 2 == 0
    first = [(i, i ^ 1) for i in range(size)]
    second = []
    for i in range(1, size, 2):
        if ring or i + 1 < size:
            second += [(i, (i + 1) % size), ((i + 1) % size, i)]
    return lax.ppermute(low, axis, first), lax.ppermute(high, axis, second)


def exchanged(block):
    return lax.all_to_all(block, ("lat", "lon"), 0, 0, tiled=True)


def local(forcing, depth, mask, guess):
    rows, cols = depth.shape
    count = cols // 128 + 1
    total = rows + 4 * HALO
    fields = FS + 2
    peers = lax.axis_size("lat") * lax.axis_size("lon")
    field = (count, total, 128)

    own = (fields, count - 1, rows, 128)
    own_fields, *ends = call(
        tile_kernel, [own] + [(fields * HALO, cols)] * 2, [], (depth, mask, forcing, guess), "tile"
    )
    low, high = swapped(*ends, "lat", False)
    vectors = -(-fields * (rows // 8 + 2) // 16)
    packs = call(pack_kernel, [(8 * vectors, 128)] * 2, [], (own_fields, low, high), "pack")
    low_col, high_col = swapped(*packs, "lon", True)
    held, extra, sums = call(
        relax_kernel,
        [(START + FS + 1,) + field, (len(EXTRA), count - 1, rows, 128), (peers, 8, 128)],
        [((FS + 1) * (FS + 2) // 2,) + field, field, (1024, 128)],
        (own_fields, low, high, low_col, high_col),
        "relax",
    )
    here, offset, kept = call(
        slab_kernel, [field, field, (8, 128)], [(1,) + field] * 2, (exchanged(sums), held), "slab"
    )
    slabs = lax.axis_size("tm")
    back = [(i, i - 1) for i in range(1, slabs)]
    moved = lax.ppermute(here, "tm", back)
    is_final = lax.axis_index("tm") == slabs - 1
    spare_place = (count - 1, TOP, SPARE)
    for _ in range(slabs - 2):
        factor = jnp.where(is_final, kept[2, 0], moved[spare_place])
        upper = jnp.where(is_final, held[START], moved)
        here, parts = call(
            chain_kernel,
            [field, (2, 8, 128)],
            [],
            (upper, held, offset, jnp.full((8, 128), factor)),
            "chain",
        )
        norm, curve = lax.psum((jnp.sum(parts[0]), jnp.sum(parts[1])), ("lat", "lon"))
        here = here.at[count - 1, :, SPARE].set(norm / (norm + FS * curve + EPSILON))
        moved = lax.ppermute(here, "tm", back)
    upper, sums = call(
        moment_kernel,
        [field, (peers, 8, 128)],
        [(FS,) + field, (1024, 128)],
        (moved, held, extra),
        "moment",
    )
    (out,) = call(
        correct_kernel,
        [(FS, rows, cols)],
        [(1,) + field] * 2,
        (exchanged(sums), kept, upper, held, offset),
        "correct",
    )
    return out


def solution(mesh):
    return jax.shard_map(
        local,
        mesh=mesh,
        in_specs=(P("tm", "lat", "lon"), P("lat", "lon"), P("lat", "lon"), P("tm", "lat", "lon")),
        out_specs=P("tm", "lat", "lon"),
        check_vma=False,
    )
```

```python
import functools
import math
import jax
import jax.numpy as jnp
from jax import lax
from jax.experimental import pallas as pl
from jax.experimental.pallas import tpu as pltpu
from jax.sharding import PartitionSpec as P

FS = 4
COUPLING = 3.0
EPSILON = 1e-06
HALO = 8
TOP = 2 * HALO

LENGTHS_RELAX = {
    (i, j): (2 * (FS + 1) - i - j if i or j else 2 * FS + 2) for i in range(FS + 1) for j in range(i, FS + 1)
}
LENGTHS_CORRECT = {(0, j): 2 * FS - j for j in range(FS - 1)}
SPARE_BYTES = 2 << 20
VMEM_BYTES = 67043328
EDGE_ROOM = 57344
SPARE = 64


def offsets_of(lengths):
    places, at = {}, 0
    for pair, length in lengths.items():
        places[pair] = at
        at += length
    return places


PLACES_RELAX = offsets_of(LENGTHS_RELAX)
PLACES_CORRECT = offsets_of(LENGTHS_CORRECT)


def two_sum(a, b):
    s = a + b
    t = s - a
    return s, (a - (s - t)) + (b - t)


def quick_sum(a, b):
    s = a + b
    return s, b - (s - a)


def pair_add(x, y):
    s, e = two_sum(x[0], y[0])
    return quick_sum(s, e + (x[1] + y[1]))


def split(a):
    t = 4097.0 * a
    hi = t - (t - a)
    return hi, a - hi


def pair_scale(x, d):
    p = x[0] * d
    ah, al = split(x[0])
    bh, bl = split(d)
    e = ((ah * bh - p) + ah * bl + al * bh) + al * bl
    return quick_sum(p, e + x[1] * d)


def tree(items):
    while len(items) > 1:
        items = [pair_add(items[i], items[i + 1]) if i + 1 < len(items) else items[i] for i in range(0, len(items), 2)]
    return items[0]


def roll_pair(x, shift, axis):
    return tuple(pltpu.roll(part, shift, axis) for part in x)


def spread_first(x):
    return jnp.broadcast_to(x[0:1, 0:1], (8, 128))


EAST, WEST, NORTH, START = 0, 1, 2, 3


def lap_rows(src, held, row, tiles):
    count = held.shape[1]
    lane = lax.broadcasted_iota(jnp.int32, (8, 128), 1)
    last, first = lane == 127, lane == 0
    here, below, above = pl.ds(row, 8), pl.ds(row + 1, 8), pl.ds(row - 1, 8)
    v = [src[c, here, :] for c in range(count)]
    left = [pltpu.roll(x, 1, 1) for x in v]
    right = [pltpu.roll(x, 127, 1) for x in v]
    out = []
    for c in range(tiles):
        e = held[EAST, c, here, :] * (v[c] - jnp.where(last, right[(c + 1) % count], right[c]))
        w = held[WEST, c, here, :] * (v[c] - jnp.where(first, left[(c - 1) % count], left[c]))
        n = held[NORTH, c, here, :] * (v[c] - src[c, below, :])
        s = held[NORTH, c, above, :] * (v[c] - src[c, above, :])
        out.append((e + w) + (n + s))
    return out


def zero_spare(ref, lead, rows):
    for k in range(lead):
        for c in range(ref.shape[1]):
            ref[k, c, pl.ds(0, 8), :] = jnp.zeros((8, 128), jnp.float32)
            ref[k, c, pl.ds(rows - 8, 8), :] = jnp.zeros((8, 128), jnp.float32)


def dot_groups(acc, groups, load, rows, tiles):
    for group in groups:
        keys = sorted({k for _, a, b in group for k in (a, b)})

        def body(i, carry):
            row = pl.multiple_of(i * 8, 8)
            for c in range(tiles):
                held = {k: load(k, c, row) for k in keys}
                carry = tuple(old + held[a] * held[b] for old, (_, a, b) in zip(carry, group))
            return carry

        sums = lax.fori_loop(
            0, rows // 8, body, tuple(jnp.zeros((8, 128), jnp.float32) for _ in group)
        )
        for total, (m, _, _) in zip(sums, group):
            acc[pl.ds(8 * m, 8), :] = total


def reduce_acc(acc, count, out_ref):
    zero = jnp.zeros((128, 128), jnp.float32)
    for m in range(count, 128):
        acc[pl.ds(8 * m, 8), :] = jnp.zeros((8, 128), jnp.float32)
    hi, lo = tree([(acc[pl.ds(s, 128, stride=8), :], zero) for s in range(8)])
    hi, lo = hi.T, lo.T
    both = tree([(hi[8 * k : 8 * k + 8], lo[8 * k : 8 * k + 8]) for k in range(16)])
    for shift in (4, 2, 1):
        both = pair_add(both, roll_pair(both, shift, 0))
    sub = lax.broadcasted_iota(jnp.int32, (8, 128), 0)
    block = jnp.where(sub == 0, both[0], jnp.where(sub == 1, both[1], 0.0))
    for k in range(out_ref.shape[0]):
        out_ref[k] = block


def gather_sum(ref):
    rows = [(ref[k, 0:1, :], ref[k, 1:2, :]) for k in range(ref.shape[0])]
    hi, lo = tree(rows)
    return jnp.broadcast_to(hi, (8, 128)), jnp.broadcast_to(lo, (8, 128))


def rows_of(moments, places):
    sub = lax.broadcasted_iota(jnp.int32, (8, 128), 0)
    out = []
    for part in moments:
        built = jnp.zeros((8, 128), jnp.float32)
        for row, at in places.items():
            moved = pltpu.roll(part, (128 - at) % 128, 1) if at else part
            built = jnp.where(sub == row, moved, built)
        out.append(built)
    return tuple(out)


def fine_factors(n0, n1, n2, n3):
    den = n0 + n1 + EPSILON
    a0 = n0 / den
    left = (n1 + EPSILON) / den
    s1 = jnp.maximum(left * left * n0 - 2.0 * left * a0 * n1 + a0 * a0 * n2, 0.0)
    big = left + s1 / (n0 + EPSILON)
    small = -a0
    curve = big * big * (n0 + n1) + 2.0 * big * small * (n1 + n2) + small * small * (n2 + n3)
    a1 = jnp.clip(s1 / (curve + EPSILON), 0.0, 1.0)
    return a0 + a1 * big, a1 * small


def coarse_factor(state):
    n0 = state[0]
    n1 = pltpu.roll(n0, 127, 1)
    return spread_first(n0 / (n0 + FS * n1 + EPSILON))


def factors_of(state):
    n0 = state[0]
    d0, d1 = fine_factors(n0, pltpu.roll(n0, 127, 1), pltpu.roll(n0, 126, 1), pltpu.roll(n0, 125, 1))
    return spread_first(d0), spread_first(d1)


def advance(state, gram, step, factors):
    d0, d1 = factors
    sub = lax.broadcasted_iota(jnp.int32, (8, 128), 0)

    def mixed(x, plus):
        moved = pair_add(pair_scale(x, d0), pair_scale(roll_pair(x, 127, 1), d1))
        return pair_add(moved, plus)

    def row(x, r):
        return tuple(jnp.broadcast_to(part[r : r + 1, :], (8, 128)) for part in x)

    cross = row(state, step)
    plus = tuple(jnp.where(sub == 0, a, b) for a, b in zip(cross, gram))
    half = mixed(state, plus)
    full = mixed(half, row(half, step))
    return tuple(jnp.where(sub == 0, a, b) for a, b in zip(full, half))


def gram_rows(moments, step, last):
    return rows_of(moments, {h: PLACES_RELAX[step, h] for h in range(step, last + 1)})


def edge_kernel(depth_low, depth_high, mask_low, mask_high, forcing_low, forcing_high, guess_low, guess_high, low, high):
    odd = lax.rem(lax.axis_index("lat"), 2) == 1
    for f in range(FS + 2):
        if f == 0:
            a = jnp.where(mask_low[...] > 0, depth_low[...], 0.0)
            b = jnp.where(mask_high[...] > 0, depth_high[...], 0.0)
        elif f == 1:
            a, b = guess_low[0], guess_high[0]
        else:
            a, b = forcing_low[FS + 1 - f], forcing_high[FS + 1 - f]
        low[pl.ds(8 * f, 8), :] = jnp.where(odd, a, b)
        high[pl.ds(8 * f, 8), :] = jnp.where(odd, b, a)


def tile_kernel(depth, mask, forcing, guess, own):
    for c in range(own.shape[1]):
        window = pl.ds(128 * c, 128)
        own[0, c] = jnp.where(mask[:, window] > 0, depth[:, window], 0.0)
        own[1, c] = guess[0, :, window]
        for f in range(2, FS + 2):
            own[f, c] = forcing[FS + 1 - f, :, window]


def pack_kernel(own, low_in, high_in, low_out, high_out):
    lat_odd = lax.rem(lax.axis_index("lat"), 2) == 1
    lon_odd = lax.rem(lax.axis_index("lon"), 2) == 1
    fields, tiles = own.shape[0], own.shape[2] // 8 + 2
    lane = lax.broadcasted_iota(jnp.int32, (8, 128), 1) // 8
    edges = []
    for c in (own.shape[1] - 1, 0):
        window = pl.ds(128 * c, 128)

        def tile(f, t):
            if t in (0, tiles - 1):
                a, b = low_in[pl.ds(8 * f, 8), window], high_in[pl.ds(8 * f, 8), window]
                return jnp.where(lat_odd, a, b) if t == 0 else jnp.where(lat_odd, b, a)
            return own[f, c, pl.ds(8 * (t - 1), 8), :]

        packed = [jnp.zeros((8, 128), jnp.float32) for _ in range(-(-fields * tiles // 16))]
        for f in range(fields):
            for t in range(tiles):
                at, slot = divmod(f * tiles + t, 16)
                shift = (8 * slot + (8 if c else 0)) % 128
                value = tile(f, t)
                value = pltpu.roll(value, shift, 1) if shift else value
                packed[at] = jnp.where(lane == slot, value, packed[at])
        edges.append(packed)
    for k, (e, w) in enumerate(zip(*edges)):
        low_out[pl.ds(8 * k, 8), :] = jnp.where(lon_odd, w, e)
        high_out[pl.ds(8 * k, 8), :] = jnp.where(lon_odd, e, w)


def relax_kernel(own_fields, low_in, high_in, low_col, high_col, held, extra, sums, kry, wet, acc):
    lat_odd = lax.rem(lax.axis_index("lat"), 2) == 1
    lon_odd = lax.rem(lax.axis_index("lon"), 2) == 1
    fields, own, rows, _ = own_fields.shape
    count = own + 1
    tiles = rows // 8 + 2
    total = rows + 4 * HALO
    lane = lax.broadcasted_iota(jnp.int32, (8, 128), 1)
    zero = jnp.zeros((8, 128), jnp.float32)

    def put(f, c, row, value):
        if f == 0:
            wet[c, pl.ds(row, 8), :] = value
        else:
            held[START - 1 + f, c, pl.ds(row, 8), :] = value

    start_of, at = {}, 0
    for s in range(FS + 1):
        start_of[s] = at
        at += FS + 1 - s
    zero_spare(kry, at, total)
    zero_spare(held, held.shape[0], total)
    for c in range(count):
        for row in (0, total - 8):
            wet[c, pl.ds(row, 8), :] = zero
    for f in range(fields):
        for c in range(own):
            window = pl.ds(128 * c, 128)
            a, b = low_in[pl.ds(8 * f, 8), window], high_in[pl.ds(8 * f, 8), window]
            put(f, c, TOP - 8, jnp.where(lat_odd, a, b))
            put(f, c, TOP + rows, jnp.where(lat_odd, b, a))
            for row in range(0, rows, 8):
                put(f, c, TOP + row, own_fields[f, c, pl.ds(row, 8), :])
        for t in range(tiles):
            k, slot = divmod(f * tiles + t, 16)
            a, b = low_col[pl.ds(8 * k, 8), :], high_col[pl.ds(8 * k, 8), :]
            e, w = jnp.where(lon_odd, b, a), jnp.where(lon_odd, a, b)
            e = pltpu.roll(e, 128 - 8 * slot, 1) if slot else e
            w = pltpu.roll(w, (120 - 8 * slot) % 128, 1) if slot < 15 else w
            put(f, own, TOP - 8 + 8 * t, jnp.where(lane < 8, e, jnp.where(lane >= 120, w, 0.0)))

    half = COUPLING * 0.5
    for row in range(8, total - 8, 8):
        d = [wet[c, pl.ds(row, 8), :] for c in range(count)]
        left = [pltpu.roll(x, 1, 1) for x in d]
        right = [pltpu.roll(x, 127, 1) for x in d]
        for c in range(count):
            sides = (
                (EAST, jnp.where(lane == 127, right[(c + 1) % count], right[c])),
                (WEST, jnp.where(lane == 0, left[(c - 1) % count], left[c])),
                (NORTH, wet[c, pl.ds(row + 1, 8), :]),
            )
            for place, other in sides:
                held[place, c, pl.ds(row, 8), :] = jnp.where((d[c] > 0) & (other > 0), half * (d[c] + other), 0.0)

    def source(s, degree):
        return kry.at[start_of[s] + degree - 1] if degree else held.at[START + s]

    for degree in range(FS + 1):
        for s in range(FS + 1 - degree):
            final = s + degree == FS
            src, dst = source(s, degree), source(s, degree + 1)
            for row in range(TOP, TOP + rows, 8) if final else range(8, total - 8, 8):
                for c, value in enumerate(lap_rows(src, held, row, own if final else count)):
                    dst[c, pl.ds(row, 8), :] = value

    for k, (s, degree) in enumerate(EXTRA):
        for c in range(own):
            extra[k, c] = source(s, degree)[c, pl.ds(TOP, rows), :]

    groups, group = [], []
    for (i, j), length in LENGTHS_RELAX.items():
        if len(group) + length > 26:
            groups.append(group)
            group = []
        for k in range(length):
            b = min(k // 2, FS + 1 - j)
            group.append((PLACES_RELAX[i, j] + k, (i, k - b), (j, b)))
    groups.append(group)
    dot_groups(acc, groups, lambda key, c, row: source(*key)[c, pl.ds(row + TOP, 8), :], rows, own)
    reduce_acc(acc, sum(LENGTHS_RELAX.values()), sums)


EXTRA = ((1, 1), (1, 2), (2, 1))


def sent_size(own, rows):
    tiles = rows // 8 + 1
    columns = own * tiles
    return columns, columns + tiles // 16 + 1


def pack_sent(sent, value, own, rows):
    sub = lax.broadcasted_iota(jnp.int32, (8, 128), 0)
    lane = lax.broadcasted_iota(jnp.int32, (8, 128), 1) // 8
    columns, size = sent_size(own, rows)
    packed = [jnp.zeros((8, 128), jnp.float32) for _ in range(size - columns)]
    for t in range(rows // 8 + 1):
        for c in range(own + 1):
            if t < rows // 8:
                x = value(c, TOP + 8 * t)
            else:
                x = pltpu.roll(jnp.where(sub < 4, value(c, TOP + rows), value(c, TOP - 8)), 4, 0)
            if c < own:
                sent[own * t + c] = x
            else:
                k, slot = divmod(t, 16)
                packed[k] = jnp.where(lane == slot, pltpu.roll(x, (4 + 8 * slot) % 128, 1), packed[k])
    return packed


def unpack_sent(sent, put, own, rows):
    sub = lax.broadcasted_iota(jnp.int32, (8, 128), 0)
    lane = lax.broadcasted_iota(jnp.int32, (8, 128), 1)
    columns, size = sent_size(own, rows)
    factor = jnp.broadcast_to(sent[size - 1, 0:1, 127:128], (8, 128))
    for t in range(rows // 8 + 1):
        for c in range(own + 1):
            if c < own:
                x = sent[own * t + c]
            else:
                k, slot = divmod(t, 16)
                x = pltpu.roll(sent[columns + k], (124 - 8 * slot) % 128, 1)
                x = jnp.where((lane < 4) | (lane >= 124), x, jnp.where(lane == SPARE, factor, 0.0))
            if t < rows // 8:
                put(c, TOP + 8 * t, x)
            else:
                x = pltpu.roll(x, 4, 0)
                put(c, TOP - 8, jnp.where(sub < 4, 0.0, x))
                put(c, TOP + rows, jnp.where(sub < 4, x, 0.0))
    return factor


def slab_kernel(gathered, held, sent, offset, kept, one, two):
    rows = held.shape[2]
    count = held.shape[1]
    lane = lax.broadcasted_iota(jnp.int32, (8, 128), 1)
    sub = lax.broadcasted_iota(jnp.int32, (8, 128), 0)
    moments = gather_sum(gathered)
    state = rows_of(moments, {j: PLACES_RELAX[0, j] for j in range(FS + 1)})
    down = coarse_factor(state)
    steps = []
    for step in range(1, FS + 1):
        factors = factors_of(state)
        steps.append(factors)
        state = advance(state, gram_rows(moments, step, FS), step, factors)
    lifted = coarse_factor(state)
    kept[...] = jnp.where(sub == 0, moments[0], jnp.where(sub == 1, moments[1], jnp.where(sub == 2, down, 0.0)))
    for ref in (one, two):
        zero_spare(ref, 1, rows)
    zero = jnp.zeros((8, 128), jnp.float32)
    for c in range(count):
        for row in (0, rows - 8):
            offset[c, pl.ds(row, 8), :] = zero
    sources = [held.at[START], one.at[0], two.at[0], one.at[0]]
    for step, (d0, d1) in enumerate(steps):
        src = sources[step]
        for row in range(8, rows - 8, 8):
            window = pl.ds(row, 8)
            for c, value in enumerate(lap_rows(src, held, row, count)):
                value = d0 * src[c, window, :] + d1 * value + held[START + 1 + step, c, window, :]
                if step < FS - 1:
                    sources[step + 1][c, window, :] = value
                else:
                    coarse = down * held[START, c, window, :]
                    rest = value - coarse
                    offset[c, window, :] = rest
                    two[0, c, window, :] = coarse + rest
    own, inner = count - 1, rows - 2 * TOP
    columns, size = sent_size(own, inner)
    packed = pack_sent(sent, lambda c, row: two[0, c, pl.ds(row, 8), :], own, inner)
    packed[-1] = jnp.where(lane == 127, lifted, packed[-1])
    for k, x in enumerate(packed):
        sent[columns + k] = x


def moment_kernel(moved, held, extra, upper, sums, kry, acc):
    is_final = lax.axis_index("tm") == lax.axis_size("tm") - 1
    rows, count = held.shape[2], held.shape[1]
    own_rows, own = extra.shape[2], extra.shape[1]
    zero_spare(kry, FS, rows)
    zero = jnp.zeros((8, 128), jnp.float32)
    for c in range(count):
        for row in (0, rows - 8):
            upper[c, pl.ds(row, 8), :] = zero


    def put(c, row, value):
        upper[c, pl.ds(row, 8), :] = jnp.where(is_final, held[START, c, pl.ds(row, 8), :], value)

    unpack_sent(moved, put, own, own_rows)
    for degree in range(FS):
        final = degree == FS - 1
        src = kry.at[degree - 1] if degree else upper
        for row in range(TOP, TOP + own_rows, 8) if final else range(8, rows - 8, 8):
            for c, value in enumerate(lap_rows(src, held, row, own if final else count)):
                kry[degree, c, pl.ds(row, 8), :] = value

    def load(key, c, row):
        s, degree = key
        if s == 0:
            return (kry.at[degree - 1] if degree else upper)[c, pl.ds(row + TOP, 8), :]
        if degree == 0:
            return held[START + s, c, pl.ds(row + TOP, 8), :]
        return extra[EXTRA.index(key), c, pl.ds(row, 8), :]

    group = []
    for (i, j), length in LENGTHS_CORRECT.items():
        for k in range(length):
            b = max(k - FS, 0) if j else k // 2
            group.append((PLACES_CORRECT[i, j] + k, (0, k - b), (j, b)))
    dot_groups(acc, [group], load, own_rows, own)
    reduce_acc(acc, sum(LENGTHS_CORRECT.values()), sums)


def correct_kernel(gathered, kept, upper, held, offset, result, one, two, out, left):
    is_final = lax.axis_index("tm") == lax.axis_size("tm") - 1
    rows, count = held.shape[2], held.shape[1]
    own_rows, own = out.shape[1], out.shape[2] // 128
    moments = gather_sum(gathered)
    before = tuple(jnp.broadcast_to(kept[k : k + 1, :], (8, 128)) for k in range(2))
    state = rows_of(moments, {j: PLACES_CORRECT[0, j] for j in range(FS - 1)})
    steps = []
    for step in range(1, FS):
        factors = factors_of(state)
        steps.append(factors)
        if step < FS - 1:
            state = advance(state, gram_rows(before, step, FS - 2), step, factors)
    down = jnp.broadcast_to(kept[2:3, :], (8, 128))
    lifted = jnp.broadcast_to(upper[count - 1, pl.ds(TOP, 8), :][0:1, SPARE : SPARE + 1], (8, 128))
    factor = jnp.where(is_final, down, lifted)
    for ref in (one, two):
        zero_spare(ref, 1, rows)
    sources, copies = [upper, one.at[0], two.at[0]], []
    for step, (d0, d1) in enumerate(steps):
        src, level, final = sources[step], FS - 1 - step, step == FS - 2
        for row in range(TOP, TOP + own_rows, 8) if final else range(8, rows - 8, 8):
            window, to_row = pl.ds(row, 8), pl.ds(row - TOP, 8)
            inside = TOP <= row < TOP + own_rows
            for c, value in enumerate(lap_rows(src, held, row, own if final else count)):
                lanes = pl.ds(128 * c, 128)
                value = d0 * src[c, window, :] + d1 * value + held[START + 1 + step, c, window, :]
                if not final:
                    sources[step + 1][c, window, :] = value
                if inside and c < own:
                    out[level, to_row, lanes] = value
                    if step == 0:
                        out[0, to_row, lanes] = factor * upper[c, window, :] + offset[c, window, :]
        for k in (level, 0) if step == 0 else (level,):
            copies.append(pltpu.make_async_copy(out.at[k], result.at[k], left.at[k]))
            copies[-1].start()
    for copy in copies:
        copy.wait()


def chain_kernel(moved, held, offset, kept, sent, sums, here):
    is_final = lax.axis_index("tm") == lax.axis_size("tm") - 1
    rows, count = held.shape[2], held.shape[1]
    own, inner = count - 1, rows - 2 * TOP
    zero = jnp.zeros((8, 128), jnp.float32)
    for c in range(count):
        for row in (0, rows - 8):
            here[c, pl.ds(row, 8), :] = zero

    def put(c, row, value):
        here[c, pl.ds(row, 8), :] = jnp.where(is_final, held[START, c, pl.ds(row, 8), :], value)

    factor = jnp.where(is_final, jnp.broadcast_to(kept[2:3, :], (8, 128)), unpack_sent(moved, put, own, inner))
    for row in range(8, rows - 8, 8):
        for c in range(count):
            window = pl.ds(row, 8)
            here[c, window, :] = factor * here[c, window, :] + offset[c, window, :]
    columns, _ = sent_size(own, inner)
    for k, x in enumerate(pack_sent(sent, lambda c, row: here[c, pl.ds(row, 8), :], own, inner)):
        sent[columns + k] = x
    plain = curved = zero
    for row in range(TOP, rows - TOP, 8):
        for c, image in enumerate(lap_rows(here, held, row, own)):
            value = here[c, pl.ds(row, 8), :]
            plain, curved = plain + value * value, curved + value * image
    sums[0], sums[1] = plain, curved


def call(kernel, outs, scratch, args, name, to_hbm=False):
    scratch = [x if hasattr(x, "dtype") else pltpu.VMEM(x, jnp.float32) for x in scratch]
    limit = sum(math.prod(x.shape) * 4 for x in scratch) + sum(math.prod(shape) * 4 for shape in outs)
    return pl.pallas_call(
        kernel,
        out_shape=tuple(jax.ShapeDtypeStruct(shape, jnp.float32) for shape in outs),
        in_specs=[pl.BlockSpec(memory_space=pltpu.VMEM)] * len(args),
        out_specs=tuple(pl.BlockSpec(memory_space=pl.ANY if to_hbm else pltpu.VMEM) for _ in outs),
        scratch_shapes=scratch,
        compiler_params=pltpu.CompilerParams(vmem_limit_bytes=limit + sum(x.size * 4 for x in args) + SPARE_BYTES),
        name=name,
    )(*args)


def edges(forcing, depth, mask, guess):
    rows, cols = depth.shape
    last = rows // HALO - 1
    specs, args = [], []
    for x in (depth, mask, forcing, guess):
        lead = x.shape[:-2]
        for at in (0, last):
            specs.append(pl.BlockSpec(lead + (HALO, cols), lambda i, lead=lead, at=at: (0,) * len(lead) + (at, 0)))
            args.append(x)
    shape = ((FS + 2) * HALO, cols)
    return pl.pallas_call(
        edge_kernel,
        grid=(1,),
        out_shape=(jax.ShapeDtypeStruct(shape, jnp.float32),) * 2,
        in_specs=specs,
        out_specs=(pl.BlockSpec(shape, lambda i: (0, 0)),) * 2,
        compiler_params=pltpu.CompilerParams(vmem_limit_bytes=VMEM_BYTES - 2 * math.prod(shape) * 4 - EDGE_ROOM),
        name="edges",
    )(*args)


def swapped(low, high, axis, ring):
    size = lax.axis_size(axis)
    assert size % 2 == 0
    first = [(i, i ^ 1) for i in range(size)]
    second = []
    for i in range(1, size, 2):
        if ring or i + 1 < size:
            second += [(i, (i + 1) % size), ((i + 1) % size, i)]
    return lax.ppermute(low, axis, first), lax.ppermute(high, axis, second)


def exchanged(block):
    return lax.all_to_all(block, ("lat", "lon"), 0, 0, tiled=True)


def local(forcing, depth, mask, guess):
    rows, cols = depth.shape
    count = cols // 128 + 1
    total = rows + 4 * HALO
    fields = FS + 2
    peers = lax.axis_size("lat") * lax.axis_size("lon")
    field = (count, total, 128)

    own = (fields, count - 1, rows, 128)
    low, high = swapped(*edges(forcing, depth, mask, guess), "lat", False)
    (own_fields,) = call(tile_kernel, [own], [], (depth, mask, forcing, guess), "tile")
    vectors = -(-fields * (rows // 8 + 2) // 16)
    packs = call(pack_kernel, [(8 * vectors, 128)] * 2, [], (own_fields, low, high), "pack")
    low_col, high_col = swapped(*packs, "lon", True)
    held, extra, sums = call(
        relax_kernel,
        [(START + FS + 1,) + field, (len(EXTRA), count - 1, rows, 128), (peers, 8, 128)],
        [((FS + 1) * (FS + 2) // 2,) + field, field, (1024, 128)],
        (own_fields, low, high, low_col, high_col),
        "relax",
    )
    _, size = sent_size(count - 1, rows)
    here, offset, kept = call(
        slab_kernel,
        [(size, 8, 128), field, (8, 128)],
        [(1,) + field] * 2,
        (exchanged(sums), held),
        "slab",
    )
    slabs = lax.axis_size("tm")
    back = [(i, i - 1) for i in range(1, slabs)]
    moved = lax.ppermute(here, "tm", back)
    for _ in range(slabs - 2):
        here, parts = call(chain_kernel, [(size, 8, 128), (2, 8, 128)], [field], (moved, held, offset, kept), "chain")
        norm, curve = lax.psum((jnp.sum(parts[0]), jnp.sum(parts[1])), ("lat", "lon"))
        here = here.at[size - 1, :, 127].set(norm / (norm + FS * curve + EPSILON))
        moved = lax.ppermute(here, "tm", back)
    upper, sums = call(
        moment_kernel,
        [field, (peers, 8, 128)],
        [(FS,) + field, (1024, 128)],
        (moved, held, extra),
        "moment",
    )
    (out,) = call(
        correct_kernel,
        [(FS, rows, cols)],
        [(1,) + field] * 2 + [(FS, rows, cols), pltpu.SemaphoreType.DMA((FS,))],
        (exchanged(sums), kept, upper, held, offset),
        "correct",
        to_hbm=True,
    )
    return out


def solution(mesh):
    return jax.shard_map(
        local,
        mesh=mesh,
        in_specs=(P("tm", "lat", "lon"), P("lat", "lon"), P("lat", "lon"), P("tm", "lat", "lon")),
        out_specs=P("tm", "lat", "lon"),
        check_vma=False,
    )
```

```python
import functools
import math
import jax
import jax.numpy as jnp
from jax import lax
from jax.experimental import pallas as pl
from jax.experimental.pallas import tpu as pltpu
from jax.sharding import PartitionSpec as P

FS = 4
COUPLING = 3.0
EPSILON = 1e-06
HALO = 8
TOP = 2 * HALO

LENGTHS_RELAX = {
    (i, j): (2 * (FS + 1) - i - j if i or j else 2 * FS + 2) for i in range(FS + 1) for j in range(i, FS + 1)
}
LENGTHS_CORRECT = {(0, j): 2 * FS - j for j in range(FS - 1)}
SPARE_BYTES = 2 << 20
VMEM_BYTES = 67043328
EDGE_ROOM = 57344
SPARE = 64


def offsets_of(lengths):
    places, at = {}, 0
    for pair, length in lengths.items():
        places[pair] = at
        at += length
    return places


PLACES_RELAX = offsets_of(LENGTHS_RELAX)
PLACES_CORRECT = offsets_of(LENGTHS_CORRECT)


def two_sum(a, b):
    s = a + b
    t = s - a
    return s, (a - (s - t)) + (b - t)


def quick_sum(a, b):
    s = a + b
    return s, b - (s - a)


def pair_add(x, y):
    s, e = two_sum(x[0], y[0])
    return quick_sum(s, e + (x[1] + y[1]))


def split(a):
    t = 4097.0 * a
    hi = t - (t - a)
    return hi, a - hi


def pair_scale(x, d):
    p = x[0] * d
    ah, al = split(x[0])
    bh, bl = split(d)
    e = ((ah * bh - p) + ah * bl + al * bh) + al * bl
    return quick_sum(p, e + x[1] * d)


def tree(items):
    while len(items) > 1:
        items = [pair_add(items[i], items[i + 1]) if i + 1 < len(items) else items[i] for i in range(0, len(items), 2)]
    return items[0]


def roll_pair(x, shift, axis):
    return tuple(pltpu.roll(part, shift, axis) for part in x)


def spread_first(x):
    return jnp.broadcast_to(x[0:1, 0:1], (8, 128))


EAST, NORTH, START = 0, 1, 2
WEST, LAST = 0, 1


def lap_rows(src, held, west, row, tiles):
    count = held.shape[1]
    lane = lax.broadcasted_iota(jnp.int32, (8, 128), 1)
    last, first = lane == 127, lane == 0
    here, below, above = pl.ds(row, 8), pl.ds(row + 1, 8), pl.ds(row - 1, 8)
    v = [src[c, here, :] for c in range(count)]
    left = [pltpu.roll(x, 1, 1) for x in v]
    right = [pltpu.roll(x, 127, 1) for x in v]
    out = []
    for c in range(tiles):
        e = held[EAST, c, here, :] * (v[c] - jnp.where(last, right[(c + 1) % count], right[c]))
        w = west[c, here, :] * (v[c] - jnp.where(first, left[(c - 1) % count], left[c]))
        n = held[NORTH, c, here, :] * (v[c] - src[c, below, :])
        s = held[NORTH, c, above, :] * (v[c] - src[c, above, :])
        out.append((e + w) + (n + s))
    return out


def zero_spare(ref, lead, rows):
    for k in range(lead):
        for c in range(ref.shape[1]):
            ref[k, c, pl.ds(0, 8), :] = jnp.zeros((8, 128), jnp.float32)
            ref[k, c, pl.ds(rows - 8, 8), :] = jnp.zeros((8, 128), jnp.float32)


def dot_groups(acc, groups, load, rows, tiles):
    for group in groups:
        keys = sorted({k for _, a, b in group for k in (a, b)})

        def body(i, carry):
            row = pl.multiple_of(i * 8, 8)
            for c in range(tiles):
                held = {k: load(k, c, row) for k in keys}
                carry = tuple(old + held[a] * held[b] for old, (_, a, b) in zip(carry, group))
            return carry

        sums = lax.fori_loop(
            0, rows // 8, body, tuple(jnp.zeros((8, 128), jnp.float32) for _ in group)
        )
        for total, (m, _, _) in zip(sums, group):
            acc[pl.ds(8 * m, 8), :] = total


def reduce_acc(acc, count, out_ref):
    zero = jnp.zeros((128, 128), jnp.float32)
    for m in range(count, 128):
        acc[pl.ds(8 * m, 8), :] = jnp.zeros((8, 128), jnp.float32)
    hi, lo = tree([(acc[pl.ds(s, 128, stride=8), :], zero) for s in range(8)])
    hi, lo = hi.T, lo.T
    both = tree([(hi[8 * k : 8 * k + 8], lo[8 * k : 8 * k + 8]) for k in range(16)])
    for shift in (4, 2, 1):
        both = pair_add(both, roll_pair(both, shift, 0))
    sub = lax.broadcasted_iota(jnp.int32, (8, 128), 0)
    block = jnp.where(sub == 0, both[0], jnp.where(sub == 1, both[1], 0.0))
    for k in range(out_ref.shape[0]):
        out_ref[k] = block[0:2, :]


def gather_sum(ref, start, count):
    rows = [(ref[start + k, 0:1, :], ref[start + k, 1:2, :]) for k in range(count)]
    hi, lo = tree(rows)
    return jnp.broadcast_to(hi, (8, 128)), jnp.broadcast_to(lo, (8, 128))


def rows_of(moments, places):
    sub = lax.broadcasted_iota(jnp.int32, (8, 128), 0)
    out = []
    for part in moments:
        built = jnp.zeros((8, 128), jnp.float32)
        for row, at in places.items():
            moved = pltpu.roll(part, (128 - at) % 128, 1) if at else part
            built = jnp.where(sub == row, moved, built)
        out.append(built)
    return tuple(out)


def fine_factors(n0, n1, n2, n3):
    den = n0 + n1 + EPSILON
    a0 = n0 / den
    left = (n1 + EPSILON) / den
    s1 = jnp.maximum(left * left * n0 - 2.0 * left * a0 * n1 + a0 * a0 * n2, 0.0)
    big = left + s1 / (n0 + EPSILON)
    small = -a0
    curve = big * big * (n0 + n1) + 2.0 * big * small * (n1 + n2) + small * small * (n2 + n3)
    a1 = jnp.clip(s1 / (curve + EPSILON), 0.0, 1.0)
    return a0 + a1 * big, a1 * small


def coarse_factor(state):
    n0 = state[0]
    n1 = pltpu.roll(n0, 127, 1)
    return spread_first(n0 / (n0 + FS * n1 + EPSILON))


def factors_of(state):
    n0 = state[0]
    d0, d1 = fine_factors(n0, pltpu.roll(n0, 127, 1), pltpu.roll(n0, 126, 1), pltpu.roll(n0, 125, 1))
    return spread_first(d0), spread_first(d1)


def advance(state, gram, step, factors):
    d0, d1 = factors
    sub = lax.broadcasted_iota(jnp.int32, (8, 128), 0)

    def mixed(x, plus):
        moved = pair_add(pair_scale(x, d0), pair_scale(roll_pair(x, 127, 1), d1))
        return pair_add(moved, plus)

    def row(x, r):
        return tuple(jnp.broadcast_to(part[r : r + 1, :], (8, 128)) for part in x)

    cross = row(state, step)
    plus = tuple(jnp.where(sub == 0, a, b) for a, b in zip(cross, gram))
    half = mixed(state, plus)
    full = mixed(half, row(half, step))
    return tuple(jnp.where(sub == 0, a, b) for a, b in zip(full, half))


def gram_rows(moments, step, last):
    return rows_of(moments, {h: PLACES_RELAX[step, h] for h in range(step, last + 1)})


def edge_kernel(depth_low, depth_high, mask_low, mask_high, forcing_low, forcing_high, guess_low, guess_high, low, high):
    odd = lax.rem(lax.axis_index("lat"), 2) == 1
    for f in range(FS + 2):
        if f == 0:
            a = jnp.where(mask_low[...] > 0, depth_low[...], 0.0)
            b = jnp.where(mask_high[...] > 0, depth_high[...], 0.0)
        elif f == 1:
            a, b = guess_low[0], guess_high[0]
        else:
            a, b = forcing_low[FS + 1 - f], forcing_high[FS + 1 - f]
        low[pl.ds(8 * f, 8), :] = jnp.where(odd, a, b)
        high[pl.ds(8 * f, 8), :] = jnp.where(odd, b, a)


def tile_kernel(depth, mask, forcing, guess, own):
    for c in range(own.shape[1]):
        window = pl.ds(128 * c, 128)
        own[0, c] = jnp.where(mask[:, window] > 0, depth[:, window], 0.0)
        own[1, c] = guess[0, :, window]
        for f in range(2, FS + 2):
            own[f, c] = forcing[FS + 1 - f, :, window]


def pack_kernel(own, low_in, high_in, low_out, high_out):
    lat_odd = lax.rem(lax.axis_index("lat"), 2) == 1
    lon_odd = lax.rem(lax.axis_index("lon"), 2) == 1
    fields, tiles = own.shape[0], own.shape[2] // 8 + 2
    lane = lax.broadcasted_iota(jnp.int32, (8, 128), 1) // 8
    edges = []
    for c in (own.shape[1] - 1, 0):
        window = pl.ds(128 * c, 128)

        def tile(f, t):
            if t in (0, tiles - 1):
                a, b = low_in[pl.ds(8 * f, 8), window], high_in[pl.ds(8 * f, 8), window]
                return jnp.where(lat_odd, a, b) if t == 0 else jnp.where(lat_odd, b, a)
            return own[f, c, pl.ds(8 * (t - 1), 8), :]

        packed = [jnp.zeros((8, 128), jnp.float32) for _ in range(-(-fields * tiles // 16))]
        for f in range(fields):
            for t in range(tiles):
                at, slot = divmod(f * tiles + t, 16)
                shift = (8 * slot + (8 if c else 0)) % 128
                value = tile(f, t)
                value = pltpu.roll(value, shift, 1) if shift else value
                packed[at] = jnp.where(lane == slot, value, packed[at])
        edges.append(packed)
    for k, (e, w) in enumerate(zip(*edges)):
        low_out[pl.ds(8 * k, 8), :] = jnp.where(lon_odd, w, e)
        high_out[pl.ds(8 * k, 8), :] = jnp.where(lon_odd, e, w)


def build_kernel(own_fields, low_in, high_in, low_col, high_col, held, tail, ahead, wet):
    lat_odd = lax.rem(lax.axis_index("lat"), 2) == 1
    lon_odd = lax.rem(lax.axis_index("lon"), 2) == 1
    fields, own, rows, _ = own_fields.shape
    count = own + 1
    tiles = rows // 8 + 2
    total = rows + 4 * HALO
    lane = lax.broadcasted_iota(jnp.int32, (8, 128), 1)
    zero = jnp.zeros((8, 128), jnp.float32)

    def put(f, c, row, value):
        if f == 0:
            wet[c, pl.ds(row, 8), :] = value
        else:
            (tail.at[LAST] if f == FS + 1 else held.at[START - 1 + f])[c, pl.ds(row, 8), :] = value

    zero_spare(held, held.shape[0], total)
    zero_spare(tail, 2, total)
    for c in range(count):
        for row in (0, total - 8):
            wet[c, pl.ds(row, 8), :] = zero
    for f in range(fields):
        for c in range(own):
            window = pl.ds(128 * c, 128)
            a, b = low_in[pl.ds(8 * f, 8), window], high_in[pl.ds(8 * f, 8), window]
            put(f, c, TOP - 8, jnp.where(lat_odd, a, b))
            put(f, c, TOP + rows, jnp.where(lat_odd, b, a))
            for row in range(0, rows, 8):
                put(f, c, TOP + row, own_fields[f, c, pl.ds(row, 8), :])
        for t in range(tiles):
            k, slot = divmod(f * tiles + t, 16)
            a, b = low_col[pl.ds(8 * k, 8), :], high_col[pl.ds(8 * k, 8), :]
            e, w = jnp.where(lon_odd, b, a), jnp.where(lon_odd, a, b)
            e = pltpu.roll(e, 128 - 8 * slot, 1) if slot else e
            w = pltpu.roll(w, (120 - 8 * slot) % 128, 1) if slot < 15 else w
            put(f, own, TOP - 8 + 8 * t, jnp.where(lane < 8, e, jnp.where(lane >= 120, w, 0.0)))

    half = COUPLING * 0.5
    for row in range(8, total - 8, 8):
        d = [wet[c, pl.ds(row, 8), :] for c in range(count)]
        left = [pltpu.roll(x, 1, 1) for x in d]
        right = [pltpu.roll(x, 127, 1) for x in d]
        for c in range(count):
            sides = (
                (held.at[EAST], jnp.where(lane == 127, right[(c + 1) % count], right[c])),
                (tail.at[WEST], jnp.where(lane == 0, left[(c - 1) % count], left[c])),
                (held.at[NORTH], wet[c, pl.ds(row + 1, 8), :]),
            )
            for place, other in sides:
                place[c, pl.ds(row, 8), :] = jnp.where((d[c] > 0) & (other > 0), half * (d[c] + other), 0.0)

    _, size = sent_size(own, rows)
    for k in range(FS - 2):
        part, field = ahead.at[pl.ds(size * k, size)], held.at[START + 1 + k]
        for at, x in enumerate(pack_sent(part, lambda c, row: field[c, pl.ds(row, 8), :], own, rows)):
            part[own * (rows // 8 + 1) + at] = x


def relax_kernel(held, tail, sums, *rest):
    *extra, kry, acc = rest
    total, count = held.shape[2], held.shape[1]
    own, rows = count - 1, total - 2 * TOP
    start_of, at = {}, 0
    for s in range(FS + 1):
        start_of[s] = at
        at += FS + 1 - s
    zero_spare(kry, at, total)

    def source(s, degree):
        if degree:
            return kry.at[start_of[s] + degree - 1]
        return tail.at[LAST] if s == FS else held.at[START + s]

    for degree in range(FS + 1):
        for s in range(FS + 1 - degree):
            final = s + degree == FS
            src, dst = source(s, degree), source(s, degree + 1)
            for row in range(TOP, TOP + rows, 8) if final else range(8, total - 8, 8):
                for c, value in enumerate(lap_rows(src, held, tail.at[WEST], row, own if final else count)):
                    dst[c, pl.ds(row, 8), :] = value

    for k, (s, degree) in enumerate(EXTRA if extra else ()):
        for c in range(own):
            extra[0][k, c] = source(s, degree)[c, pl.ds(TOP, rows), :]

    groups, group = [], []
    for (i, j), length in LENGTHS_RELAX.items():
        if len(group) + length > 26:
            groups.append(group)
            group = []
        for k in range(length):
            b = min(k // 2, FS + 1 - j)
            group.append((PLACES_RELAX[i, j] + k, (i, k - b), (j, b)))
    groups.append(group)
    dot_groups(acc, groups, lambda key, c, row: source(*key)[c, pl.ds(row + TOP, 8), :], rows, own)
    reduce_acc(acc, sum(LENGTHS_RELAX.values()), sums)


EXTRA = ((1, 1), (1, 2), (2, 1))


def sent_size(own, rows):
    tiles = rows // 8 + 1
    columns = own * tiles
    return columns, columns + tiles // 16 + 1


def pack_sent(sent, value, own, rows):
    sub = lax.broadcasted_iota(jnp.int32, (8, 128), 0)
    lane = lax.broadcasted_iota(jnp.int32, (8, 128), 1) // 8
    columns, size = sent_size(own, rows)
    packed = [jnp.zeros((8, 128), jnp.float32) for _ in range(size - columns)]
    for t in range(rows // 8 + 1):
        for c in range(own + 1):
            if t < rows // 8:
                x = value(c, TOP + 8 * t)
            else:
                x = pltpu.roll(jnp.where(sub < 4, value(c, TOP + rows), value(c, TOP - 8)), 4, 0)
            if c < own:
                sent[own * t + c] = x
            else:
                k, slot = divmod(t, 16)
                packed[k] = jnp.where(lane == slot, pltpu.roll(x, (4 + 8 * slot) % 128, 1), packed[k])
    return packed


def unpack_sent(sent, put, own, rows):
    sub = lax.broadcasted_iota(jnp.int32, (8, 128), 0)
    lane = lax.broadcasted_iota(jnp.int32, (8, 128), 1)
    columns, size = sent_size(own, rows)
    factor = jnp.broadcast_to(sent[size - 1, 0:1, 127:128], (8, 128))
    for t in range(rows // 8 + 1):
        for c in range(own + 1):
            if c < own:
                x = sent[own * t + c]
            else:
                k, slot = divmod(t, 16)
                x = pltpu.roll(sent[columns + k], (124 - 8 * slot) % 128, 1)
                x = jnp.where((lane < 4) | (lane >= 124), x, jnp.where(lane == SPARE, factor, 0.0))
            if t < rows // 8:
                put(c, TOP + 8 * t, x)
            else:
                x = pltpu.roll(x, 4, 0)
                put(c, TOP - 8, jnp.where(sub < 4, 0.0, x))
                put(c, TOP + rows, jnp.where(sub < 4, x, 0.0))
    return factor


def slab_kernel(gathered, held, tail, sent, here, offset, kept, one, two):
    rows = held.shape[2]
    count = held.shape[1]
    own, inner = count - 1, rows - 2 * TOP
    lane = lax.broadcasted_iota(jnp.int32, (8, 128), 1)
    sub = lax.broadcasted_iota(jnp.int32, (8, 128), 0)
    moments = gather_sum(gathered, 0, gathered.shape[0])
    state = rows_of(moments, {j: PLACES_RELAX[0, j] for j in range(FS + 1)})
    down = coarse_factor(state)
    steps = []
    for step in range(1, FS + 1):
        factors = factors_of(state)
        steps.append(factors)
        state = advance(state, gram_rows(moments, step, FS), step, factors)
    lifted = coarse_factor(state)
    kept[...] = jnp.where(sub == 0, moments[0], jnp.where(sub == 1, moments[1], jnp.where(sub == 2, down, 0.0)))
    for ref in (one, two):
        zero_spare(ref, 1, rows)
    zero = jnp.zeros((8, 128), jnp.float32)
    for c in range(count):
        for row in (0, rows - 8):
            here[c, pl.ds(row, 8), :] = zero
    sources = [held.at[START], one.at[0], two.at[0], one.at[0]]
    for step, (d0, d1) in enumerate(steps):
        src = sources[step]
        for row in range(8, rows - 8, 8):
            window = pl.ds(row, 8)
            for c, value in enumerate(lap_rows(src, held, tail.at[WEST], row, count)):
                term = held.at[START + 1 + step] if step < FS - 1 else tail.at[LAST]
                value = d0 * src[c, window, :] + d1 * value + term[c, window, :]
                if step < FS - 1:
                    sources[step + 1][c, window, :] = value
                else:
                    coarse = down * held[START, c, window, :]
                    rest = value - coarse
                    if offset.shape[0] == count:
                        offset[c, window, :] = rest
                    elif c < own and TOP <= row < rows - TOP:
                        offset[c, pl.ds(row - TOP, 8), :] = rest
                    here[c, window, :] = coarse + rest
    columns, size = sent_size(own, inner)
    packed = pack_sent(sent, lambda c, row: here[c, pl.ds(row, 8), :], own, inner)
    packed[-1] = jnp.where(lane == 127, lifted, packed[-1])
    for k, x in enumerate(packed):
        sent[columns + k] = x


def moment_kernel(moved, held, tail, extra, upper, sums, kry, acc):
    is_final = lax.axis_index("tm") == lax.axis_size("tm") - 1
    rows, count = held.shape[2], held.shape[1]
    own_rows, own = extra.shape[2], extra.shape[1]
    zero_spare(kry, FS, rows)
    zero = jnp.zeros((8, 128), jnp.float32)
    for c in range(count):
        for row in (0, rows - 8):
            upper[c, pl.ds(row, 8), :] = zero


    def put(c, row, value):
        upper[c, pl.ds(row, 8), :] = jnp.where(is_final, held[START, c, pl.ds(row, 8), :], value)

    unpack_sent(moved, put, own, own_rows)
    for degree in range(FS):
        final = degree == FS - 1
        src = kry.at[degree - 1] if degree else upper
        for row in range(TOP, TOP + own_rows, 8) if final else range(8, rows - 8, 8):
            for c, value in enumerate(lap_rows(src, held, tail.at[WEST], row, own if final else count)):
                kry[degree, c, pl.ds(row, 8), :] = value

    def load(key, c, row):
        s, degree = key
        if s == 0:
            return (kry.at[degree - 1] if degree else upper)[c, pl.ds(row + TOP, 8), :]
        if degree == 0:
            return held[START + s, c, pl.ds(row + TOP, 8), :]
        return extra[EXTRA.index(key), c, pl.ds(row, 8), :]

    group = []
    for (i, j), length in LENGTHS_CORRECT.items():
        for k in range(length):
            b = max(k - FS, 0) if j else k // 2
            group.append((PLACES_CORRECT[i, j] + k, (0, k - b), (j, b)))
    dot_groups(acc, [group], load, own_rows, own)
    reduce_acc(acc, sum(LENGTHS_CORRECT.values()), sums)


def sender_kernel(here, held, tail, ahead, sums, kry, acc):
    rows, count = held.shape[2], held.shape[1]
    own, own_rows = count - 1, rows - 2 * TOP
    _, size = sent_size(own, own_rows)
    keys = [(0, k) for k in range(1, FS + 1)] + [(1, 0), (1, 1), (1, 2), (2, 0), (2, 1)]
    place = {key: kry.at[k] for k, key in enumerate(keys)}
    place[0, 0] = here
    zero_spare(kry, len(keys), rows)
    for j in range(1, FS - 1):
        field = place[j, 0]

        def put(c, row, value):
            field[c, pl.ds(row, 8), :] = value

        unpack_sent(ahead.at[pl.ds(size * (j - 1), size)], put, own, own_rows)
    for key in keys:
        s, degree = key
        if not degree:
            continue
        final = (s, degree + 1) not in place
        for row in range(TOP, TOP + own_rows, 8) if final else range(8, rows - 8, 8):
            for c, value in enumerate(lap_rows(place[s, degree - 1], held, tail.at[WEST], row, own if final else count)):
                place[key][c, pl.ds(row, 8), :] = value
    group = []
    for (i, j), length in LENGTHS_CORRECT.items():
        for k in range(length):
            b = max(k - FS, 0) if j else k // 2
            group.append((PLACES_CORRECT[i, j] + k, (0, k - b), (j, b)))
    dot_groups(acc, [group], lambda key, c, row: place[key][c, pl.ds(row + TOP, 8), :], own_rows, own)
    reduce_acc(acc, sum(LENGTHS_CORRECT.values()), sums)


def correct_kernel(direct, gathered, kept, moved, held, offset, result, one, two, out, left, west, *upper):
    me, slabs = lax.axis_index("tm"), lax.axis_size("tm")
    is_final = me == slabs - 1
    rows, count = held.shape[2], held.shape[1]
    own_rows, own = out.shape[1], out.shape[2] // 128
    before = tuple(jnp.broadcast_to(kept[k : k + 1, :], (8, 128)) for k in range(2))
    down = jnp.broadcast_to(kept[2:3, :], (8, 128))
    peers = gathered.shape[0] // slabs if direct else gathered.shape[0]
    moments = gather_sum(gathered, jnp.minimum(me + 1, slabs - 1) * peers if direct else 0, peers)
    state = rows_of(moments, {j: PLACES_CORRECT[0, j] for j in range(FS - 1)})
    if direct:
        same = rows_of(before, {j: PLACES_RELAX[0, j] for j in range(FS - 1)})
        state = tuple(jnp.where(is_final, a, b) for a, b in zip(same, state))
        (upper,) = upper
        zero = jnp.zeros((8, 128), jnp.float32)
        for c in range(count):
            for row in (0, rows - 8):
                upper[c, pl.ds(row, 8), :] = zero

        def put(c, row, value):
            upper[c, pl.ds(row, 8), :] = jnp.where(is_final, held[START, c, pl.ds(row, 8), :], value)

        lifted = unpack_sent(moved, put, own, own_rows)
    else:
        upper = moved
        lifted = jnp.broadcast_to(upper[count - 1, pl.ds(TOP, 8), :][0:1, SPARE : SPARE + 1], (8, 128))
    factor = jnp.where(is_final, down, lifted)
    lane = lax.broadcasted_iota(jnp.int32, (8, 128), 1)
    for row in range(8, rows - 8, 8):
        turned = [pltpu.roll(held[EAST, c, pl.ds(row, 8), :], 1, 1) for c in range(count)]
        for c in range(count):
            west[c, pl.ds(row, 8), :] = jnp.where(lane == 0, turned[(c - 1) % count], turned[c])
    steps = []
    for step in range(1, FS):
        factors = factors_of(state)
        steps.append(factors)
        if step < FS - 1:
            state = advance(state, gram_rows(before, step, FS - 2), step, factors)
    for ref in (one, two):
        zero_spare(ref, 1, rows)
    sources, copies = [upper, one.at[0], two.at[0]], []
    for step, (d0, d1) in enumerate(steps):
        src, level, final = sources[step], FS - 1 - step, step == FS - 2
        for row in range(TOP, TOP + own_rows, 8) if final else range(8, rows - 8, 8):
            window, to_row = pl.ds(row, 8), pl.ds(row - TOP, 8)
            part = to_row if direct else window
            inside = TOP <= row < TOP + own_rows
            for c, value in enumerate(lap_rows(src, held, west, row, own if final else count)):
                lanes = pl.ds(128 * c, 128)
                value = d0 * src[c, window, :] + d1 * value + held[START + 1 + step, c, window, :]
                if not final:
                    sources[step + 1][c, window, :] = value
                if inside and c < own:
                    out[level, to_row, lanes] = value
                    if step == 0:
                        out[0, to_row, lanes] = factor * upper[c, window, :] + offset[c, part, :]
        for k in (level, 0) if step == 0 else (level,):
            copies.append(pltpu.make_async_copy(out.at[k], result.at[k], left.at[k]))
            copies[-1].start()
    for copy in copies:
        copy.wait()


def chain_kernel(moved, held, tail, offset, kept, sent, sums, here):
    is_final = lax.axis_index("tm") == lax.axis_size("tm") - 1
    rows, count = held.shape[2], held.shape[1]
    own, inner = count - 1, rows - 2 * TOP
    zero = jnp.zeros((8, 128), jnp.float32)
    for c in range(count):
        for row in (0, rows - 8):
            here[c, pl.ds(row, 8), :] = zero

    def put(c, row, value):
        here[c, pl.ds(row, 8), :] = jnp.where(is_final, held[START, c, pl.ds(row, 8), :], value)

    factor = jnp.where(is_final, jnp.broadcast_to(kept[2:3, :], (8, 128)), unpack_sent(moved, put, own, inner))
    for row in range(8, rows - 8, 8):
        for c in range(count):
            window = pl.ds(row, 8)
            here[c, window, :] = factor * here[c, window, :] + offset[c, window, :]
    columns, _ = sent_size(own, inner)
    for k, x in enumerate(pack_sent(sent, lambda c, row: here[c, pl.ds(row, 8), :], own, inner)):
        sent[columns + k] = x
    plain = curved = zero
    for row in range(TOP, rows - TOP, 8):
        for c, image in enumerate(lap_rows(here, held, tail.at[WEST], row, own)):
            value = here[c, pl.ds(row, 8), :]
            plain, curved = plain + value * value, curved + value * image
    sums[0], sums[1] = plain, curved


def call(kernel, outs, scratch, args, name, to_hbm=False):
    scratch = [x if hasattr(x, "dtype") else pltpu.VMEM(x, jnp.float32) for x in scratch]
    limit = sum(math.prod(x.shape) * 4 for x in scratch) + sum(math.prod(shape) * 4 for shape in outs)
    return pl.pallas_call(
        kernel,
        out_shape=tuple(jax.ShapeDtypeStruct(shape, jnp.float32) for shape in outs),
        in_specs=[pl.BlockSpec(memory_space=pltpu.VMEM)] * len(args),
        out_specs=tuple(pl.BlockSpec(memory_space=pl.ANY if to_hbm else pltpu.VMEM) for _ in outs),
        scratch_shapes=scratch,
        compiler_params=pltpu.CompilerParams(vmem_limit_bytes=limit + sum(x.size * 4 for x in args) + SPARE_BYTES),
        name=name,
    )(*args)


def edges(forcing, depth, mask, guess):
    rows, cols = depth.shape
    last = rows // HALO - 1
    specs, args = [], []
    for x in (depth, mask, forcing, guess):
        lead = x.shape[:-2]
        for at in (0, last):
            specs.append(pl.BlockSpec(lead + (HALO, cols), lambda i, lead=lead, at=at: (0,) * len(lead) + (at, 0)))
            args.append(x)
    shape = ((FS + 2) * HALO, cols)
    return pl.pallas_call(
        edge_kernel,
        grid=(1,),
        out_shape=(jax.ShapeDtypeStruct(shape, jnp.float32),) * 2,
        in_specs=specs,
        out_specs=(pl.BlockSpec(shape, lambda i: (0, 0)),) * 2,
        compiler_params=pltpu.CompilerParams(vmem_limit_bytes=VMEM_BYTES - 2 * math.prod(shape) * 4 - EDGE_ROOM),
        name="edges",
    )(*args)


def swapped(low, high, axis, ring):
    size = lax.axis_size(axis)
    assert size % 2 == 0
    first = [(i, i ^ 1) for i in range(size)]
    second = []
    for i in range(1, size, 2):
        if ring or i + 1 < size:
            second += [(i, (i + 1) % size), ((i + 1) % size, i)]
    return lax.ppermute(low, axis, first), lax.ppermute(high, axis, second)


def exchanged(block, axes=("lat", "lon")):
    return lax.all_to_all(block, axes, 0, 0, tiled=True)


def local(forcing, depth, mask, guess):
    rows, cols = depth.shape
    count = cols // 128 + 1
    total = rows + 4 * HALO
    fields = FS + 2
    peers = lax.axis_size("lat") * lax.axis_size("lon")
    field, own = (count, total, 128), (count - 1, rows, 128)

    low, high = swapped(*edges(forcing, depth, mask, guess), "lat", False)
    (own_fields,) = call(tile_kernel, [(fields,) + own], [], (depth, mask, forcing, guess), "tile")
    vectors = -(-fields * (rows // 8 + 2) // 16)
    packs = call(pack_kernel, [(8 * vectors, 128)] * 2, [], (own_fields, low, high), "pack")
    low_col, high_col = swapped(*packs, "lon", True)
    _, size = sent_size(count - 1, rows)
    slabs = lax.axis_size("tm")
    direct = slabs == 2
    held, tail, ahead = call(
        build_kernel,
        [(START + FS,) + field, (2,) + field, (size * (FS - 2), 8, 128)],
        [field],
        (own_fields, low, high, low_col, high_col),
        "build",
    )
    if direct:
        with jax.named_scope("ahead"):
            ahead = lax.ppermute(ahead, "tm", [(i, i + 1) for i in range(slabs - 1)])
    with jax.named_scope("relax"):
        sums, *extra = call(
            relax_kernel,
            [(peers, 2, 128)] + ([] if direct else [(len(EXTRA),) + own]),
            [((FS + 1) * (FS + 2) // 2,) + field, (1024, 128)],
            (held, tail),
            "relax",
        )
    sent, here, offset, kept = call(
        slab_kernel,
        [(size, 8, 128), field, own if direct else field, (8, 128)],
        [(1,) + field] * 2,
        (exchanged(sums), held, tail),
        "slab",
    )
    back = [(i, i - 1) for i in range(1, slabs)]
    with jax.named_scope("back"):
        moved = lax.ppermute(sent, "tm", back)
    scratch = [(1,) + field] * 2 + [(FS, rows, cols), pltpu.SemaphoreType.DMA((FS,)), field]
    if direct:
        with jax.named_scope("sender"):
            (sums,) = call(
                sender_kernel,
                [(slabs * peers, 2, 128)],
                [(FS + 5,) + field, (1024, 128)],
                (here, held, tail, ahead),
                "sender",
            )
        gathered, start = exchanged(sums, ("tm", "lat", "lon")), moved
        scratch.append(field)
    else:
        for _ in range(slabs - 2):
            sent, parts = call(
                chain_kernel, [(size, 8, 128), (2, 8, 128)], [field], (moved, held, tail, offset, kept), "chain"
            )
            norm, curve = lax.psum((jnp.sum(parts[0]), jnp.sum(parts[1])), ("lat", "lon"))
            sent = sent.at[size - 1, :, 127].set(norm / (norm + FS * curve + EPSILON))
            moved = lax.ppermute(sent, "tm", back)
        start, sums = call(
            moment_kernel,
            [field, (peers, 2, 128)],
            [(FS,) + field, (1024, 128)],
            (moved, held, tail, *extra),
            "moment",
        )
        gathered = exchanged(sums)
    (out,) = call(
        functools.partial(correct_kernel, direct),
        [(FS, rows, cols)],
        scratch,
        (gathered, kept, start, held, offset),
        "correct",
        to_hbm=True,
    )
    return out


def solution(mesh):
    return jax.shard_map(
        local,
        mesh=mesh,
        in_specs=(P("tm", "lat", "lon"), P("lat", "lon"), P("lat", "lon"), P("tm", "lat", "lon")),
        out_specs=P("tm", "lat", "lon"),
        check_vma=False,
    )
```

```python
import functools
import math
import jax
import jax.numpy as jnp
from jax import lax
from jax.experimental import pallas as pl
from jax.experimental.pallas import tpu as pltpu
from jax.sharding import PartitionSpec as P

FS = 4
COUPLING = 3.0
EPSILON = 1e-06
HALO = 8
TOP = 2 * HALO

LENGTHS_RELAX = {
    (i, j): (2 * (FS + 1) - i - j if i or j else 2 * FS + 2) for i in range(FS + 1) for j in range(i, FS + 1)
}
LENGTHS_CORRECT = {(0, j): 2 * FS - j for j in range(FS - 1)}
SPARE_BYTES = 2 << 20
VMEM_BYTES = 67043328
EDGE_ROOM = 57344
SPARE = 64


def offsets_of(lengths):
    places, at = {}, 0
    for pair, length in lengths.items():
        places[pair] = at
        at += length
    return places


PLACES_RELAX = offsets_of(LENGTHS_RELAX)
PLACES_CORRECT = offsets_of(LENGTHS_CORRECT)


def two_sum(a, b):
    s = a + b
    t = s - a
    return s, (a - (s - t)) + (b - t)


def quick_sum(a, b):
    s = a + b
    return s, b - (s - a)


def pair_add(x, y):
    s, e = two_sum(x[0], y[0])
    return quick_sum(s, e + (x[1] + y[1]))


def split(a):
    t = 4097.0 * a
    hi = t - (t - a)
    return hi, a - hi


def pair_scale(x, d):
    p = x[0] * d
    ah, al = split(x[0])
    bh, bl = split(d)
    e = ((ah * bh - p) + ah * bl + al * bh) + al * bl
    return quick_sum(p, e + x[1] * d)


def tree(items):
    while len(items) > 1:
        items = [pair_add(items[i], items[i + 1]) if i + 1 < len(items) else items[i] for i in range(0, len(items), 2)]
    return items[0]


def roll_pair(x, shift, axis):
    return tuple(pltpu.roll(part, shift, axis) for part in x)


def spread_first(x):
    return jnp.broadcast_to(x[0:1, 0:1], (8, 128))


EAST, NORTH, START = 0, 1, 2
WEST, LAST = 0, 1


def lap_rows(src, held, west, row, tiles):
    count = held.shape[1]
    lane = lax.broadcasted_iota(jnp.int32, (8, 128), 1)
    last, first = lane == 127, lane == 0
    here, below, above = pl.ds(row, 8), pl.ds(row + 1, 8), pl.ds(row - 1, 8)
    v = [src[c, here, :] for c in range(count)]
    left = [pltpu.roll(x, 1, 1) for x in v]
    right = [pltpu.roll(x, 127, 1) for x in v]
    out = []
    for c in range(tiles):
        e = held[EAST, c, here, :] * (v[c] - jnp.where(last, right[(c + 1) % count], right[c]))
        w = west[c, here, :] * (v[c] - jnp.where(first, left[(c - 1) % count], left[c]))
        n = held[NORTH, c, here, :] * (v[c] - src[c, below, :])
        s = held[NORTH, c, above, :] * (v[c] - src[c, above, :])
        out.append((e + w) + (n + s))
    return out


def zero_spare(ref, lead, rows):
    for k in range(lead):
        for c in range(ref.shape[1]):
            ref[k, c, pl.ds(0, 8), :] = jnp.zeros((8, 128), jnp.float32)
            ref[k, c, pl.ds(rows - 8, 8), :] = jnp.zeros((8, 128), jnp.float32)


def dot_groups(acc, groups, load, rows, tiles):
    for group in groups:
        keys = sorted({k for _, a, b in group for k in (a, b)})

        def body(i, carry):
            row = pl.multiple_of(i * 8, 8)
            for c in range(tiles):
                held = {k: load(k, c, row) for k in keys}
                carry = tuple(old + held[a] * held[b] for old, (_, a, b) in zip(carry, group))
            return carry

        sums = lax.fori_loop(
            0, rows // 8, body, tuple(jnp.zeros((8, 128), jnp.float32) for _ in group)
        )
        for total, (m, _, _) in zip(sums, group):
            acc[pl.ds(8 * m, 8), :] = total


def reduce_acc(acc, count, out_ref):
    zero = jnp.zeros((128, 128), jnp.float32)
    for m in range(count, 128):
        acc[pl.ds(8 * m, 8), :] = jnp.zeros((8, 128), jnp.float32)
    hi, lo = tree([(acc[pl.ds(s, 128, stride=8), :], zero) for s in range(8)])
    hi, lo = hi.T, lo.T
    both = tree([(hi[8 * k : 8 * k + 8], lo[8 * k : 8 * k + 8]) for k in range(16)])
    for shift in (4, 2, 1):
        both = pair_add(both, roll_pair(both, shift, 0))
    sub = lax.broadcasted_iota(jnp.int32, (8, 128), 0)
    block = jnp.where(sub == 0, both[0], jnp.where(sub == 1, both[1], 0.0))
    for k in range(out_ref.shape[0]):
        out_ref[k] = block[0:2, :]


def gather_sum(ref, start, count):
    rows = [(ref[start + k, 0:1, :], ref[start + k, 1:2, :]) for k in range(count)]
    hi, lo = tree(rows)
    return jnp.broadcast_to(hi, (8, 128)), jnp.broadcast_to(lo, (8, 128))


def rows_of(moments, places):
    sub = lax.broadcasted_iota(jnp.int32, (8, 128), 0)
    out = []
    for part in moments:
        built = jnp.zeros((8, 128), jnp.float32)
        for row, at in places.items():
            moved = pltpu.roll(part, (128 - at) % 128, 1) if at else part
            built = jnp.where(sub == row, moved, built)
        out.append(built)
    return tuple(out)


def fine_factors(n0, n1, n2, n3):
    den = n0 + n1 + EPSILON
    a0 = n0 / den
    left = (n1 + EPSILON) / den
    s1 = jnp.maximum(left * left * n0 - 2.0 * left * a0 * n1 + a0 * a0 * n2, 0.0)
    big = left + s1 / (n0 + EPSILON)
    small = -a0
    curve = big * big * (n0 + n1) + 2.0 * big * small * (n1 + n2) + small * small * (n2 + n3)
    a1 = jnp.clip(s1 / (curve + EPSILON), 0.0, 1.0)
    return a0 + a1 * big, a1 * small


def coarse_factor(state):
    n0 = state[0]
    n1 = pltpu.roll(n0, 127, 1)
    return spread_first(n0 / (n0 + FS * n1 + EPSILON))


def factors_of(state):
    n0 = state[0]
    d0, d1 = fine_factors(n0, pltpu.roll(n0, 127, 1), pltpu.roll(n0, 126, 1), pltpu.roll(n0, 125, 1))
    return spread_first(d0), spread_first(d1)


def advance(state, gram, step, factors):
    d0, d1 = factors
    sub = lax.broadcasted_iota(jnp.int32, (8, 128), 0)

    def mixed(x, plus):
        moved = pair_add(pair_scale(x, d0), pair_scale(roll_pair(x, 127, 1), d1))
        return pair_add(moved, plus)

    def row(x, r):
        return tuple(jnp.broadcast_to(part[r : r + 1, :], (8, 128)) for part in x)

    cross = row(state, step)
    plus = tuple(jnp.where(sub == 0, a, b) for a, b in zip(cross, gram))
    half = mixed(state, plus)
    full = mixed(half, row(half, step))
    return tuple(jnp.where(sub == 0, a, b) for a, b in zip(full, half))


def gram_rows(moments, step, last):
    return rows_of(moments, {h: PLACES_RELAX[step, h] for h in range(step, last + 1)})


def edge_kernel(depth_low, depth_high, mask_low, mask_high, forcing_low, forcing_high, guess_low, guess_high, low, high):
    odd = lax.rem(lax.axis_index("lat"), 2) == 1
    for f in range(FS + 2):
        if f == 0:
            a = jnp.where(mask_low[...] > 0, depth_low[...], 0.0)
            b = jnp.where(mask_high[...] > 0, depth_high[...], 0.0)
        elif f == 1:
            a, b = guess_low[0], guess_high[0]
        else:
            a, b = forcing_low[FS + 1 - f], forcing_high[FS + 1 - f]
        low[pl.ds(8 * f, 8), :] = jnp.where(odd, a, b)
        high[pl.ds(8 * f, 8), :] = jnp.where(odd, b, a)


def tile_kernel(depth, mask, forcing, guess, own):
    for c in range(own.shape[1]):
        window = pl.ds(128 * c, 128)
        own[0, c] = jnp.where(mask[:, window] > 0, depth[:, window], 0.0)
        own[1, c] = guess[0, :, window]
        for f in range(2, FS + 2):
            own[f, c] = forcing[FS + 1 - f, :, window]


def pack_kernel(own, low_in, high_in, low_out, high_out):
    lat_odd = lax.rem(lax.axis_index("lat"), 2) == 1
    lon_odd = lax.rem(lax.axis_index("lon"), 2) == 1
    fields, tiles = own.shape[0], own.shape[2] // 8 + 2
    lane = lax.broadcasted_iota(jnp.int32, (8, 128), 1) // 8
    edges = []
    for c in (own.shape[1] - 1, 0):
        window = pl.ds(128 * c, 128)

        def tile(f, t):
            if t in (0, tiles - 1):
                a, b = low_in[pl.ds(8 * f, 8), window], high_in[pl.ds(8 * f, 8), window]
                return jnp.where(lat_odd, a, b) if t == 0 else jnp.where(lat_odd, b, a)
            return own[f, c, pl.ds(8 * (t - 1), 8), :]

        packed = [jnp.zeros((8, 128), jnp.float32) for _ in range(-(-fields * tiles // 16))]
        for f in range(fields):
            for t in range(tiles):
                at, slot = divmod(f * tiles + t, 16)
                shift = (8 * slot + (8 if c else 0)) % 128
                value = tile(f, t)
                value = pltpu.roll(value, shift, 1) if shift else value
                packed[at] = jnp.where(lane == slot, value, packed[at])
        edges.append(packed)
    for k, (e, w) in enumerate(zip(*edges)):
        low_out[pl.ds(8 * k, 8), :] = jnp.where(lon_odd, w, e)
        high_out[pl.ds(8 * k, 8), :] = jnp.where(lon_odd, e, w)


def build_kernel(own_fields, low_in, high_in, low_col, high_col, held, tail, ahead, wet):
    lat_odd = lax.rem(lax.axis_index("lat"), 2) == 1
    lon_odd = lax.rem(lax.axis_index("lon"), 2) == 1
    fields, own, rows, _ = own_fields.shape
    count = own + 1
    tiles = rows // 8 + 2
    total = rows + 4 * HALO
    lane = lax.broadcasted_iota(jnp.int32, (8, 128), 1)
    zero = jnp.zeros((8, 128), jnp.float32)

    def put(f, c, row, value):
        if f == 0:
            wet[c, pl.ds(row, 8), :] = value
        else:
            (tail.at[LAST] if f == FS + 1 else held.at[START - 1 + f])[c, pl.ds(row, 8), :] = value

    zero_spare(held, held.shape[0], total)
    zero_spare(tail, 2, total)
    for c in range(count):
        for row in (0, total - 8):
            wet[c, pl.ds(row, 8), :] = zero
    for f in range(fields):
        for c in range(own):
            window = pl.ds(128 * c, 128)
            a, b = low_in[pl.ds(8 * f, 8), window], high_in[pl.ds(8 * f, 8), window]
            put(f, c, TOP - 8, jnp.where(lat_odd, a, b))
            put(f, c, TOP + rows, jnp.where(lat_odd, b, a))
            for row in range(0, rows, 8):
                put(f, c, TOP + row, own_fields[f, c, pl.ds(row, 8), :])
        for t in range(tiles):
            k, slot = divmod(f * tiles + t, 16)
            a, b = low_col[pl.ds(8 * k, 8), :], high_col[pl.ds(8 * k, 8), :]
            e, w = jnp.where(lon_odd, b, a), jnp.where(lon_odd, a, b)
            e = pltpu.roll(e, 128 - 8 * slot, 1) if slot else e
            w = pltpu.roll(w, (120 - 8 * slot) % 128, 1) if slot < 15 else w
            put(f, own, TOP - 8 + 8 * t, jnp.where(lane < 8, e, jnp.where(lane >= 120, w, 0.0)))

    half = COUPLING * 0.5
    for row in range(8, total - 8, 8):
        d = [wet[c, pl.ds(row, 8), :] for c in range(count)]
        left = [pltpu.roll(x, 1, 1) for x in d]
        right = [pltpu.roll(x, 127, 1) for x in d]
        for c in range(count):
            sides = (
                (held.at[EAST], jnp.where(lane == 127, right[(c + 1) % count], right[c])),
                (tail.at[WEST], jnp.where(lane == 0, left[(c - 1) % count], left[c])),
                (held.at[NORTH], wet[c, pl.ds(row + 1, 8), :]),
            )
            for place, other in sides:
                place[c, pl.ds(row, 8), :] = jnp.where((d[c] > 0) & (other > 0), half * (d[c] + other), 0.0)

    _, size = sent_size(own, rows)
    for k in range(FS - 2):
        part, field = ahead.at[pl.ds(size * k, size)], held.at[START + 1 + k]
        for at, x in enumerate(pack_sent(part, lambda c, row: field[c, pl.ds(row, 8), :], own, rows)):
            part[own * (rows // 8 + 1) + at] = x


def relax_kernel(held, tail, sums, *rest):
    *extra, kry, acc = rest
    total, count = held.shape[2], held.shape[1]
    own, rows = count - 1, total - 2 * TOP
    start_of, at = {}, 0
    for s in range(FS + 1):
        start_of[s] = at
        at += FS + 1 - s
    zero_spare(kry, at, total)

    def source(s, degree):
        if degree:
            return kry.at[start_of[s] + degree - 1]
        return tail.at[LAST] if s == FS else held.at[START + s]

    for degree in range(FS + 1):
        for s in range(FS + 1 - degree):
            final = s + degree == FS
            src, dst = source(s, degree), source(s, degree + 1)
            for row in range(TOP, TOP + rows, 8) if final else range(8, total - 8, 8):
                for c, value in enumerate(lap_rows(src, held, tail.at[WEST], row, own if final else count)):
                    dst[c, pl.ds(row, 8), :] = value

    for k, (s, degree) in enumerate(EXTRA if extra else ()):
        for c in range(own):
            extra[0][k, c] = source(s, degree)[c, pl.ds(TOP, rows), :]

    groups, group = [], []
    for (i, j), length in LENGTHS_RELAX.items():
        if len(group) + length > 26:
            groups.append(group)
            group = []
        for k in range(length):
            b = min(k // 2, FS + 1 - j)
            group.append((PLACES_RELAX[i, j] + k, (i, k - b), (j, b)))
    groups.append(group)
    dot_groups(acc, groups, lambda key, c, row: source(*key)[c, pl.ds(row + TOP, 8), :], rows, own)
    reduce_acc(acc, sum(LENGTHS_RELAX.values()), sums)


EXTRA = ((1, 1), (1, 2), (2, 1))


def sent_size(own, rows):
    tiles = rows // 8 + 1
    columns = own * tiles
    return columns, columns + tiles // 16 + 1


def pack_sent(sent, value, own, rows):
    sub = lax.broadcasted_iota(jnp.int32, (8, 128), 0)
    lane = lax.broadcasted_iota(jnp.int32, (8, 128), 1) // 8
    columns, size = sent_size(own, rows)
    packed = [jnp.zeros((8, 128), jnp.float32) for _ in range(size - columns)]
    for t in range(rows // 8 + 1):
        for c in range(own + 1):
            if t < rows // 8:
                x = value(c, TOP + 8 * t)
            else:
                x = pltpu.roll(jnp.where(sub < 4, value(c, TOP + rows), value(c, TOP - 8)), 4, 0)
            if c < own:
                sent[own * t + c] = x
            else:
                k, slot = divmod(t, 16)
                packed[k] = jnp.where(lane == slot, pltpu.roll(x, (4 + 8 * slot) % 128, 1), packed[k])
    return packed


def unpack_sent(sent, put, own, rows):
    sub = lax.broadcasted_iota(jnp.int32, (8, 128), 0)
    lane = lax.broadcasted_iota(jnp.int32, (8, 128), 1)
    columns, size = sent_size(own, rows)
    factor = jnp.broadcast_to(sent[size - 1, 0:1, 127:128], (8, 128))
    for t in range(rows // 8 + 1):
        for c in range(own + 1):
            if c < own:
                x = sent[own * t + c]
            else:
                k, slot = divmod(t, 16)
                x = pltpu.roll(sent[columns + k], (124 - 8 * slot) % 128, 1)
                x = jnp.where((lane < 4) | (lane >= 124), x, jnp.where(lane == SPARE, factor, 0.0))
            if t < rows // 8:
                put(c, TOP + 8 * t, x)
            else:
                x = pltpu.roll(x, 4, 0)
                put(c, TOP - 8, jnp.where(sub < 4, 0.0, x))
                put(c, TOP + rows, jnp.where(sub < 4, x, 0.0))
    return factor


def slab_kernel(gathered, held, tail, sent, here, offset, kept, one, two):
    rows = held.shape[2]
    count = held.shape[1]
    own, inner = count - 1, rows - 2 * TOP
    lane = lax.broadcasted_iota(jnp.int32, (8, 128), 1)
    sub = lax.broadcasted_iota(jnp.int32, (8, 128), 0)
    moments = gather_sum(gathered, 0, gathered.shape[0])
    state = rows_of(moments, {j: PLACES_RELAX[0, j] for j in range(FS + 1)})
    down = coarse_factor(state)
    steps = []
    for step in range(1, FS + 1):
        factors = factors_of(state)
        steps.append(factors)
        state = advance(state, gram_rows(moments, step, FS), step, factors)
    lifted = coarse_factor(state)
    kept[...] = jnp.where(sub == 0, moments[0], jnp.where(sub == 1, moments[1], jnp.where(sub == 2, down, 0.0)))
    for ref in (one, two):
        zero_spare(ref, 1, rows)
    zero = jnp.zeros((8, 128), jnp.float32)
    for c in range(count):
        for row in (0, rows - 8):
            here[c, pl.ds(row, 8), :] = zero
    sources = [held.at[START], one.at[0], two.at[0], one.at[0]]
    for step, (d0, d1) in enumerate(steps):
        src = sources[step]
        for row in range(8, rows - 8, 8):
            window = pl.ds(row, 8)
            for c, value in enumerate(lap_rows(src, held, tail.at[WEST], row, count)):
                term = held.at[START + 1 + step] if step < FS - 1 else tail.at[LAST]
                value = d0 * src[c, window, :] + d1 * value + term[c, window, :]
                if step < FS - 1:
                    sources[step + 1][c, window, :] = value
                else:
                    coarse = down * held[START, c, window, :]
                    rest = value - coarse
                    if offset.shape[0] == count:
                        offset[c, window, :] = rest
                    elif c < own and TOP <= row < rows - TOP:
                        offset[c, pl.ds(row - TOP, 8), :] = rest
                    here[c, window, :] = coarse + rest
    columns, size = sent_size(own, inner)
    packed = pack_sent(sent, lambda c, row: here[c, pl.ds(row, 8), :], own, inner)
    packed[-1] = jnp.where(lane == 127, lifted, packed[-1])
    for k, x in enumerate(packed):
        sent[columns + k] = x


def moment_kernel(moved, held, tail, extra, upper, sums, kry, acc):
    is_final = lax.axis_index("tm") == lax.axis_size("tm") - 1
    rows, count = held.shape[2], held.shape[1]
    own_rows, own = extra.shape[2], extra.shape[1]
    zero_spare(kry, FS, rows)
    zero = jnp.zeros((8, 128), jnp.float32)
    for c in range(count):
        for row in (0, rows - 8):
            upper[c, pl.ds(row, 8), :] = zero


    def put(c, row, value):
        upper[c, pl.ds(row, 8), :] = jnp.where(is_final, held[START, c, pl.ds(row, 8), :], value)

    unpack_sent(moved, put, own, own_rows)
    for degree in range(FS):
        final = degree == FS - 1
        src = kry.at[degree - 1] if degree else upper
        for row in range(TOP, TOP + own_rows, 8) if final else range(8, rows - 8, 8):
            for c, value in enumerate(lap_rows(src, held, tail.at[WEST], row, own if final else count)):
                kry[degree, c, pl.ds(row, 8), :] = value

    def load(key, c, row):
        s, degree = key
        if s == 0:
            return (kry.at[degree - 1] if degree else upper)[c, pl.ds(row + TOP, 8), :]
        if degree == 0:
            return held[START + s, c, pl.ds(row + TOP, 8), :]
        return extra[EXTRA.index(key), c, pl.ds(row, 8), :]

    group = []
    for (i, j), length in LENGTHS_CORRECT.items():
        for k in range(length):
            b = max(k - FS, 0) if j else k // 2
            group.append((PLACES_CORRECT[i, j] + k, (0, k - b), (j, b)))
    dot_groups(acc, [group], load, own_rows, own)
    reduce_acc(acc, sum(LENGTHS_CORRECT.values()), sums)


def sender_kernel(here, held, tail, ahead, sums, kry, acc):
    rows, count = held.shape[2], held.shape[1]
    own, own_rows = count - 1, rows - 2 * TOP
    _, size = sent_size(own, own_rows)
    keys = [(0, k) for k in range(1, FS + 1)] + [(1, 0), (1, 1), (1, 2), (2, 0), (2, 1)]
    place = {key: kry.at[k] for k, key in enumerate(keys)}
    place[0, 0] = here
    zero_spare(kry, len(keys), rows)
    for j in range(1, FS - 1):
        field = place[j, 0]

        def put(c, row, value):
            field[c, pl.ds(row, 8), :] = value

        unpack_sent(ahead.at[pl.ds(size * (j - 1), size)], put, own, own_rows)
    for key in keys:
        s, degree = key
        if not degree:
            continue
        final = (s, degree + 1) not in place
        for row in range(TOP, TOP + own_rows, 8) if final else range(8, rows - 8, 8):
            for c, value in enumerate(lap_rows(place[s, degree - 1], held, tail.at[WEST], row, own if final else count)):
                place[key][c, pl.ds(row, 8), :] = value
    group = []
    for (i, j), length in LENGTHS_CORRECT.items():
        for k in range(length):
            b = max(k - FS, 0) if j else k // 2
            group.append((PLACES_CORRECT[i, j] + k, (0, k - b), (j, b)))
    dot_groups(acc, [group], lambda key, c, row: place[key][c, pl.ds(row + TOP, 8), :], own_rows, own)
    reduce_acc(acc, sum(LENGTHS_CORRECT.values()), sums)


def correct_kernel(direct, gathered, kept, moved, held, offset, result, one, two, out, left, west, *upper):
    me, slabs = lax.axis_index("tm"), lax.axis_size("tm")
    is_final = me == slabs - 1
    rows, count = held.shape[2], held.shape[1]
    own_rows, own = out.shape[1], out.shape[2] // 128
    before = tuple(jnp.broadcast_to(kept[k : k + 1, :], (8, 128)) for k in range(2))
    down = jnp.broadcast_to(kept[2:3, :], (8, 128))
    peers = gathered.shape[0] // slabs if direct else gathered.shape[0]
    moments = gather_sum(gathered, jnp.minimum(me + 1, slabs - 1) * peers if direct else 0, peers)
    state = rows_of(moments, {j: PLACES_CORRECT[0, j] for j in range(FS - 1)})
    if direct:
        same = rows_of(before, {j: PLACES_RELAX[0, j] for j in range(FS - 1)})
        state = tuple(jnp.where(is_final, a, b) for a, b in zip(same, state))
        (upper,) = upper
        zero = jnp.zeros((8, 128), jnp.float32)
        for c in range(count):
            for row in (0, rows - 8):
                upper[c, pl.ds(row, 8), :] = zero

        def put(c, row, value):
            upper[c, pl.ds(row, 8), :] = jnp.where(is_final, held[START, c, pl.ds(row, 8), :], value)

        lifted = unpack_sent(moved, put, own, own_rows)
    else:
        upper = moved
        lifted = jnp.broadcast_to(upper[count - 1, pl.ds(TOP, 8), :][0:1, SPARE : SPARE + 1], (8, 128))
    factor = jnp.where(is_final, down, lifted)
    lane = lax.broadcasted_iota(jnp.int32, (8, 128), 1)
    for row in range(8, rows - 8, 8):
        turned = [pltpu.roll(held[EAST, c, pl.ds(row, 8), :], 1, 1) for c in range(count)]
        for c in range(count):
            west[c, pl.ds(row, 8), :] = jnp.where(lane == 0, turned[(c - 1) % count], turned[c])
    steps = []
    for step in range(1, FS):
        factors = factors_of(state)
        steps.append(factors)
        if step < FS - 1:
            state = advance(state, gram_rows(before, step, FS - 2), step, factors)
    for ref in (one, two):
        zero_spare(ref, 1, rows)
    sources, copies = [upper, one.at[0], two.at[0]], []
    for step, (d0, d1) in enumerate(steps):
        src, level, final = sources[step], FS - 1 - step, step == FS - 2
        for row in range(TOP, TOP + own_rows, 8) if final else range(8, rows - 8, 8):
            window, to_row = pl.ds(row, 8), pl.ds(row - TOP, 8)
            part = to_row if direct else window
            inside = TOP <= row < TOP + own_rows
            for c, value in enumerate(lap_rows(src, held, west, row, own if final else count)):
                lanes = pl.ds(128 * c, 128)
                value = d0 * src[c, window, :] + d1 * value + held[START + 1 + step, c, window, :]
                if not final:
                    sources[step + 1][c, window, :] = value
                if inside and c < own:
                    out[level, to_row, lanes] = value
                    if step == 0:
                        out[0, to_row, lanes] = factor * upper[c, window, :] + offset[c, part, :]
        for k in (level, 0) if step == 0 else (level,):
            copies.append(pltpu.make_async_copy(out.at[k], result.at[k], left.at[k]))
            copies[-1].start()
    for copy in copies:
        copy.wait()


def chain_kernel(moved, held, tail, offset, kept, sent, sums, here):
    is_final = lax.axis_index("tm") == lax.axis_size("tm") - 1
    rows, count = held.shape[2], held.shape[1]
    own, inner = count - 1, rows - 2 * TOP
    zero = jnp.zeros((8, 128), jnp.float32)
    for c in range(count):
        for row in (0, rows - 8):
            here[c, pl.ds(row, 8), :] = zero

    def put(c, row, value):
        here[c, pl.ds(row, 8), :] = jnp.where(is_final, held[START, c, pl.ds(row, 8), :], value)

    factor = jnp.where(is_final, jnp.broadcast_to(kept[2:3, :], (8, 128)), unpack_sent(moved, put, own, inner))
    for row in range(8, rows - 8, 8):
        for c in range(count):
            window = pl.ds(row, 8)
            here[c, window, :] = factor * here[c, window, :] + offset[c, window, :]
    columns, _ = sent_size(own, inner)
    for k, x in enumerate(pack_sent(sent, lambda c, row: here[c, pl.ds(row, 8), :], own, inner)):
        sent[columns + k] = x
    plain = curved = zero
    for row in range(TOP, rows - TOP, 8):
        for c, image in enumerate(lap_rows(here, held, tail.at[WEST], row, own)):
            value = here[c, pl.ds(row, 8), :]
            plain, curved = plain + value * value, curved + value * image
    sums[0], sums[1] = plain, curved


def call(kernel, outs, scratch, args, name, to_hbm=False):
    scratch = [x if hasattr(x, "dtype") else pltpu.VMEM(x, jnp.float32) for x in scratch]
    limit = sum(math.prod(x.shape) * 4 for x in scratch) + sum(math.prod(shape) * 4 for shape in outs)
    return pl.pallas_call(
        kernel,
        out_shape=tuple(jax.ShapeDtypeStruct(shape, jnp.float32) for shape in outs),
        in_specs=[pl.BlockSpec(memory_space=pltpu.VMEM)] * len(args),
        out_specs=tuple(pl.BlockSpec(memory_space=pl.ANY if to_hbm else pltpu.VMEM) for _ in outs),
        scratch_shapes=scratch,
        compiler_params=pltpu.CompilerParams(vmem_limit_bytes=limit + sum(x.size * 4 for x in args) + SPARE_BYTES),
        name=name,
    )(*args)


def edges(forcing, depth, mask, guess):
    rows, cols = depth.shape
    last = rows // HALO - 1
    specs, args = [], []
    for x in (depth, mask, forcing, guess):
        lead = x.shape[:-2]
        for at in (0, last):
            specs.append(pl.BlockSpec(lead + (HALO, cols), lambda i, lead=lead, at=at: (0,) * len(lead) + (at, 0)))
            args.append(x)
    shape = ((FS + 2) * HALO, cols)
    return pl.pallas_call(
        edge_kernel,
        grid=(1,),
        out_shape=(jax.ShapeDtypeStruct(shape, jnp.float32),) * 2,
        in_specs=specs,
        out_specs=(pl.BlockSpec(shape, lambda i: (0, 0)),) * 2,
        compiler_params=pltpu.CompilerParams(vmem_limit_bytes=VMEM_BYTES - 2 * math.prod(shape) * 4 - EDGE_ROOM),
        name="edges",
    )(*args)


def swapped(low, high, axis, ring):
    size = lax.axis_size(axis)
    assert size % 2 == 0
    first = [(i, i ^ 1) for i in range(size)]
    second = []
    for i in range(1, size, 2):
        if ring or i + 1 < size:
            second += [(i, (i + 1) % size), ((i + 1) % size, i)]
    high = lax.ppermute(high, axis, second)
    return lax.ppermute(low, axis, first), high


def exchanged(block, axes=("lat", "lon")):
    return lax.all_to_all(block, axes, 0, 0, tiled=True)


def local(forcing, depth, mask, guess):
    rows, cols = depth.shape
    count = cols // 128 + 1
    total = rows + 4 * HALO
    fields = FS + 2
    peers = lax.axis_size("lat") * lax.axis_size("lon")
    field, own = (count, total, 128), (count - 1, rows, 128)

    low, high = swapped(*edges(forcing, depth, mask, guess), "lat", False)
    (own_fields,) = call(tile_kernel, [(fields,) + own], [], (depth, mask, forcing, guess), "tile")
    vectors = -(-fields * (rows // 8 + 2) // 16)
    packs = call(pack_kernel, [(8 * vectors, 128)] * 2, [], (own_fields, low, high), "pack")
    low_col, high_col = swapped(*packs, "lon", True)
    _, size = sent_size(count - 1, rows)
    slabs = lax.axis_size("tm")
    direct = slabs == 2
    held, tail, ahead = call(
        build_kernel,
        [(START + FS,) + field, (2,) + field, (size * (FS - 2), 8, 128)],
        [field],
        (own_fields, low, high, low_col, high_col),
        "build",
    )
    if direct:
        with jax.named_scope("ahead"):
            ahead = lax.ppermute(ahead, "tm", [(i, i + 1) for i in range(slabs - 1)])
    with jax.named_scope("relax"):
        sums, *extra = call(
            relax_kernel,
            [(peers, 2, 128)] + ([] if direct else [(len(EXTRA),) + own]),
            [((FS + 1) * (FS + 2) // 2,) + field, (1024, 128)],
            (held, tail),
            "relax",
        )
    sent, here, offset, kept = call(
        slab_kernel,
        [(size, 8, 128), field, own if direct else field, (8, 128)],
        [(1,) + field] * 2,
        (exchanged(sums), held, tail),
        "slab",
    )
    back = [(i, i - 1) for i in range(1, slabs)]
    with jax.named_scope("back"):
        moved = lax.ppermute(sent, "tm", back)
    scratch = [(1,) + field] * 2 + [(FS, rows, cols), pltpu.SemaphoreType.DMA((FS,)), field]
    if direct:
        with jax.named_scope("sender"):
            (sums,) = call(
                sender_kernel,
                [(slabs * peers, 2, 128)],
                [(FS + 5,) + field, (1024, 128)],
                (here, held, tail, ahead),
                "sender",
            )
        gathered, start = exchanged(sums, ("tm", "lat", "lon")), moved
        scratch.append(field)
    else:
        for _ in range(slabs - 2):
            sent, parts = call(
                chain_kernel, [(size, 8, 128), (2, 8, 128)], [field], (moved, held, tail, offset, kept), "chain"
            )
            norm, curve = lax.psum((jnp.sum(parts[0]), jnp.sum(parts[1])), ("lat", "lon"))
            sent = sent.at[size - 1, :, 127].set(norm / (norm + FS * curve + EPSILON))
            moved = lax.ppermute(sent, "tm", back)
        start, sums = call(
            moment_kernel,
            [field, (peers, 2, 128)],
            [(FS,) + field, (1024, 128)],
            (moved, held, tail, *extra),
            "moment",
        )
        gathered = exchanged(sums)
    (out,) = call(
        functools.partial(correct_kernel, direct),
        [(FS, rows, cols)],
        scratch,
        (gathered, kept, start, held, offset),
        "correct",
        to_hbm=True,
    )
    return out


def solution(mesh):
    return jax.shard_map(
        local,
        mesh=mesh,
        in_specs=(P("tm", "lat", "lon"), P("lat", "lon"), P("lat", "lon"), P("tm", "lat", "lon")),
        out_specs=P("tm", "lat", "lon"),
        check_vma=False,
    )
```
